256 devices in a mesh: rep: 8 (over x, core), slab: 16 (over y, z_lo), pix: 2 (over z_hi).
Axes of the slice: x: 4, y: 4, z: 8 (z_hi: 2, z_lo: 4; z = z_hi * 4 + z_lo), core: 2. Of those that a mesh axis runs over, the one named last changes fastest.
Arguments:
- projections: bfloat16 [64, 256, 512], P(('rep', 'pix'), 'slab'), may hold values from -6 to 6
- ctf_weight: bfloat16 [64, 256, 256], P(('rep', 'pix'), 'slab'), may hold values from 0.099609375 to 4
- orient: int32 [64], P(('rep', 'pix')), may hold values from 0 to 63
- angle_table: int32 [64, 4, 256], replicated, may hold values from 0 to 255, as said below
Outputs:
- density: float32 [256, 256, 512], P(('rep', 'pix'), 'slab')
The draws below stay inside these ranges and needn't reach their ends.
Inputs may be any that keep to these rules, and one draw needn't show every extreme that they name: `angle_table`: for every entry and column, the lower indices lie between 3 and 253, and the fractions between 0 and 255.
All inputs are finite; a program needn't handle non-finite values.
Results may differ from the reference program's by a relative error of at most 0.0022.
Values may be sent and summed in bfloat16 or wider, within the bound.
A program may use at most 128 MiB of HBM per device.

```python
import math
import jax
import jax.numpy as jnp
from jax import lax

GRID = 256
ANGLES = 64
NPROJ = 64


def draw_angle_table(key, part):
    center = GRID // 2
    reach = 256 * (center - 3) // center
    sines = jax.random.randint(key, (ANGLES,), -reach, reach + 1)
    remain = reach * reach - sines * sines
    counter = jnp.arange(1, reach + 1, dtype=jnp.int32)
    cosines = jnp.sum((counter[None, :] * counter[None, :] <= remain[:, None]).astype(jnp.int32), axis=1)
    offsets = jnp.arange(GRID, dtype=jnp.int32) - center
    position_x = center * 256 + offsets[None, :] * cosines[:, None]
    position_z = center * 256 + offsets[None, :] * sines[:, None]
    return jnp.stack([position_x // 256, position_x % 256, position_z // 256, position_z % 256], axis=1).astype(jnp.int32)


def plant(array, stream_key, least, top_value):
    place = [jax.random.randint(jax.random.fold_in(stream_key, axis), (), 0, length) for axis, length in enumerate(array.shape)]
    widest = array.shape.index(max(array.shape))
    neighbour = place[:widest] + [(place[widest] + 1) % array.shape[widest]] + place[widest + 1:]
    return array.at[tuple(place)].set(least).at[tuple(neighbour)].set(top_value)


def level_of(rng, shape, cuts, smallest, largest):
    factor_of, own = 1.0, jax.random.fold_in(rng, 6)
    for dim, parts in cuts:
        steps = jnp.exp(jax.random.uniform(jax.random.fold_in(own, dim), (parts,), jnp.float32, smallest / len(cuts), largest / len(cuts)))
        factor_of = factor_of * jnp.repeat(steps, shape[dim] // parts).reshape([-1 if axis == dim else 1 for axis in range(len(shape))])
    return factor_of


def gaussian(stream_key, shape, spread, most, cuts=(), kind=jnp.bfloat16):
    result = jax.random.normal(stream_key, shape, jnp.float32) * spread
    if len(cuts) > 0:
        result = level_of(stream_key, shape, cuts, -0.22, 0.18) * result
    return jnp.clip(result, min=-most, max=most).astype(kind)


def setup_inputs(seed: int = 0) -> dict:
    streams_of = jax.random.split(jax.random.key(seed), 5)
    projections = gaussian(streams_of[0], (NPROJ, GRID, 2 * GRID), 1.0, 6.0, ((0, 16), (1, 16)))
    ctf_weight = jnp.clip(jnp.exp(math.log(4.0) - 3.6927934 * jax.random.uniform(streams_of[1], (NPROJ, GRID, GRID), jnp.float32) ** level_of(streams_of[1], (NPROJ, GRID, GRID), ((0, 16), (1, 16)), -0.2, 0.2)), 0.099609375, 4.0).astype(jnp.bfloat16)
    orient = plant(jax.random.randint(streams_of[2], (NPROJ,), 0, ANGLES), jax.random.fold_in(streams_of[2], 1), 0, ANGLES - 1).astype(jnp.int32)
    angle_table = draw_angle_table(jax.random.fold_in(streams_of[4], 71), 0)
    return {"projections": projections, "ctf_weight": ctf_weight, "orient": orient, "angle_table": angle_table}


def reference(projections, ctf_weight, orient, angle_table):
    samples = jnp.concatenate([projections, ctf_weight], axis=2).astype(jnp.float32)
    geometry = angle_table[orient]
    volume = jnp.zeros((GRID, GRID, 3 * GRID), jnp.float32)

    def add_one(running, item):
        rows_in, where = item
        lower_x = where[0].astype(jnp.int32)
        lower_z = where[2].astype(jnp.int32)
        share_x = where[1].astype(jnp.float32) / 256.0
        share_z = where[3].astype(jnp.float32) / 256.0
        for step_x, weight_x in ((0, 1.0 - share_x), (1, share_x)):
            for step_z, weight_z in ((0, 1.0 - share_z), (1, share_z)):
                coeff = (weight_x * weight_z).astype(jnp.bfloat16).astype(jnp.float32)
                running = running.at[lower_x + step_x, lower_z + step_z].add(coeff[:, None] * rows_in)
        return running, None

    volume, _ = lax.scan(add_one, volume, (samples, geometry))
    values = volume[:, :, :2 * GRID].reshape(GRID, GRID, 2, GRID)
    weights = volume[:, :, None, 2 * GRID:] + 1.0
    return (values / weights).reshape(GRID, GRID, 2 * GRID)
```

```python
import jax
import jax.numpy as jnp
from jax import lax
from jax.experimental import pallas as pl
from jax.experimental.pallas import tpu as pltpu
from jax.sharding import PartitionSpec as P

MESH = pl.DeviceIdType.MESH
RING = 8
STEPS_R = 4
STEPS_L = 3


def slot_r(t):
    return 2 + 4 * (t - 1)


def slot_l(t):
    return 3 + 4 * (t - 1)


def slot_pr(t):
    return 4 + 4 * (t - 1) if t < 4 else 15


def slot_pl(t):
    return 5 + 4 * (t - 1)


def kernel(
    orient_ref, proj_ref, ctf_ref, table_ref, out_ref,
    piece, landed, gath, acc, outbuf, back,
    send1, recv1, send_r, recv_r, send_l, recv_l, send_p, recv_p, send2, recv2,
):
    rep = lax.axis_index("rep")
    slab = lax.axis_index("slab")
    pix = lax.axis_index("pix")
    xc, core = rep // 2, rep % 2
    yc, zl = slab // 4, slab % 4
    zpos = pix * 4 + zl
    me = xc * 4 + yc
    sub = core * 2 + pix

    def plane(q):
        return ((q // 4) * 2 + core, (q % 4) * 4 + zl, pix)

    def along_z(step):
        z = (zpos + step + RING) % RING
        return (rep, yc * 4 + z % 4, z // 4)

    right, left = along_z(1), along_z(-1)
    partner = (xc * 2 + 1 - core, slab, pix)

    barrier = pltpu.get_barrier_semaphore()

    def greet(k, carry):
        pl.semaphore_signal(
            barrier, inc=1, device_id=plane((me + k) % 16), device_id_type=MESH
        )
        return carry

    lax.fori_loop(1, 16, greet, 0)
    for peer in (right, left, partner):
        pl.semaphore_signal(barrier, inc=1, device_id=peer, device_id_type=MESH)

    samples = proj_ref[...].reshape(64, 512).astype(jnp.float32)
    weights = ctf_ref[...].reshape(64, 256).astype(jnp.float32)
    real, imag = samples[:, :256], samples[:, 256:]
    first = jnp.concatenate([real, weights], axis=0).T
    second = jnp.concatenate([imag, imag], axis=0).T

    column = lax.broadcasted_iota(jnp.int32, (256, 128), 0)
    lane = lax.broadcasted_iota(jnp.int32, (256, 128), 1)
    geometry = jnp.zeros((4, 128), jnp.float32)
    for n in range(4):
        row = table_ref[orient_ref[n]].astype(jnp.float32).astype(jnp.bfloat16)
        pick = (column == slab * 16 + lane % 16) & ((lane // 16) % 4 == n)
        geometry += jnp.dot(
            row, pick.astype(jnp.float32).astype(jnp.bfloat16), preferred_element_type=jnp.float32
        )
    fx, fz = geometry[1:2] / 256.0, geometry[3:4] / 256.0
    facts = jnp.concatenate(
        [
            geometry[0:1],
            geometry[2:3],
            (1.0 - fx) * (1.0 - fz),
            (1.0 - fx) * fz,
            fx * (1.0 - fz),
            fx * fz,
            jnp.zeros((10, 128), jnp.float32),
        ],
        axis=0,
    )
    low_half = lax.broadcasted_iota(jnp.int32, (16, 128), 1) < 64
    for q in range(16):
        piece[q, 0:16, :] = first[16 * q : 16 * q + 16].astype(jnp.bfloat16)
        piece[q, 16:32, :] = jnp.where(
            low_half, second[16 * q : 16 * q + 16], facts
        ).astype(jnp.bfloat16)

    acc[...] = jnp.zeros_like(acc)
    pl.semaphore_wait(barrier, 18)

    def across(src, dst, send, recv, k, into):
        to = (me + k) % 16
        return pltpu.make_async_remote_copy(
            src_ref=src.at[to], dst_ref=dst.at[into], send_sem=send.at[to], recv_sem=recv.at[into],
            device_id=plane(to), device_id_type=MESH,
        )

    def start_across(*refs):
        def go(k, carry):
            across(*refs, k, me).start()
            return carry

        lax.fori_loop(1, 16, go, 0)

    def land_across(*refs):
        def go(k, carry):
            across(*refs, k, (me - k + 16) % 16).wait_recv()
            return carry

        lax.fori_loop(1, 16, go, 0)

    def drain_across(*refs):
        def go(k, carry):
            across(*refs, k, me).wait_send()
            return carry

        lax.fori_loop(1, 16, go, 0)

    start_across(piece, landed, send1, recv1)
    landed[me] = piece[me]
    land_across(piece, landed, send1, recv1)

    half = lax.broadcasted_iota(jnp.int32, (32, 128), 1) < 64
    for j in range(8):
        a = landed[2 * j].astype(jnp.float32)
        b = landed[2 * j + 1].astype(jnp.float32)
        top = jnp.where(half, a, pltpu.roll(b, 64, 1)).astype(jnp.bfloat16)
        bottom = jnp.where(half, pltpu.roll(a, 64, 1), b).astype(jnp.bfloat16)
        at = pl.ds(128 * (j % 2), 128)
        gath[j // 2, 0:32, at] = top
        gath[j // 2, 32:64, at] = bottom

    def move(src, dst, send, recv, to):
        return pltpu.make_async_remote_copy(
            src_ref=gath.at[pl.ds(4 * src, 4)], dst_ref=gath.at[pl.ds(4 * dst, 4)],
            send_sem=send, recv_sem=recv, device_id=to, device_id_type=MESH,
        )

    to_r = [move(0 if t == 1 else slot_r(t - 1), slot_r(t), send_r.at[t - 1], recv_r.at[t - 1], right)
            for t in range(1, 5)]
    to_l = [move(0 if t == 1 else slot_l(t - 1), slot_l(t), send_l.at[t - 1], recv_l.at[t - 1], left)
            for t in range(1, 4)]
    to_p = {0: move(0, 1, send_p.at[0], recv_p.at[0], partner)}
    for t in range(1, 5):
        to_p["r", t] = move(slot_r(t), slot_pr(t), send_p.at[2 * t - 1], recv_p.at[2 * t - 1], partner)
    for t in range(1, 4):
        to_p["l", t] = move(slot_l(t), slot_pl(t), send_p.at[2 * t], recv_p.at[2 * t], partner)

    row16 = lax.broadcasted_iota(jnp.int32, (16, 256), 0).astype(jnp.float32)

    def chunk(g, carry):
        block = gath[g]
        facts = block[48:64].astype(jnp.float32)
        x0 = facts[0:1].astype(jnp.int32)
        z0 = facts[1:2].astype(jnp.int32)

        def spread(v):
            return jnp.broadcast_to(v, (16, 256)).astype(jnp.bfloat16)

        total = None
        for i in range(2):
            xr = x0 + i
            x_ok = ((xr >> 4) & 3) == sub
            x_low = spread((xr & 15).astype(jnp.float32))
            keys, shares = [], []
            for j in range(2):
                zr = z0 + j
                ok = x_ok & (((zr >> 4) & 3) == zl)
                key = jnp.where(ok, (xr >> 6) * 64 + (zr >> 6) * 16 + (zr & 15), -1)
                keys.append(spread(key.astype(jnp.float32)))
                shares.append(spread(facts[2 + 2 * i + j : 3 + 2 * i + j]))
            zero = jnp.zeros((16, 256), jnp.bfloat16)
            right_side = []
            for t in range(16):
                here = (row16 + 16.0 * t).astype(jnp.bfloat16)
                right_side.append(
                    jnp.where(keys[0] == here, shares[0], jnp.where(keys[1] == here, shares[1], zero))
                )
            right_side = jnp.concatenate(right_side, axis=0)
            left_side = []
            for v in range(16):
                hit = x_low == jnp.full((16, 256), v, jnp.bfloat16)
                for c in range(3):
                    left_side.append(jnp.where(hit, block[16 * c : 16 * c + 16], zero))
            left_side = jnp.concatenate(left_side, axis=0)
            part = lax.dot_general(
                left_side, right_side, (((1,), (1,)), ((), ())), preferred_element_type=jnp.float32
            )
            total = part if total is None else total + part
        acc[...] += total
        return carry

    def compute(first_slot, count):
        lax.fori_loop(4 * first_slot, 4 * (first_slot + count), chunk, 0)

    to_r[0].start()
    to_l[0].start()
    to_p[0].start()
    compute(0, 1)
    for t in range(1, 5):
        to_r[t - 1].wait_recv()
        if t < 4:
            to_r[t].start()
        to_p["r", t].start()
        if t < 4:
            to_l[t - 1].wait_recv()
            if t < 3:
                to_l[t].start()
            to_p["l", t].start()
        if t == 1:
            to_p[0].wait_recv()
            compute(1, 3)
        else:
            to_p["r", t - 1].wait_recv()
            to_p["l", t - 1].wait_recv()
            compute(slot_pr(t - 1), 4 if t < 4 else 3)
    to_p["r", 4].wait_recv()
    compute(15, 1)

    rows = []
    for v in range(16):
        base = 48 * v
        bottom = acc[pl.ds(base + 32, 16), :] + 1.0
        rows.append(acc[pl.ds(base, 16), :] / bottom)
        rows.append(acc[pl.ds(base + 16, 16), :] / bottom)
    for m in range(4):
        turned = jnp.concatenate(rows[8 * m : 8 * m + 8], axis=0).T
        for o in range(16):
            outbuf[o, :, pl.ds(128 * m, 128)] = turned[16 * o : 16 * o + 16].astype(jnp.bfloat16)

    start_across(outbuf, back, send2, recv2)
    back[me] = outbuf[me]
    land_across(outbuf, back, send2, recv2)

    lanes = lax.broadcasted_iota(jnp.int32, (16, 128), 1) // 16
    for m in range(4):
        for high in range(2):
            tiles = [back[8 * high + k, :, pl.ds(128 * m, 128)].astype(jnp.float32) for k in range(8)]
            for bit in (1, 2, 4):
                clear = (lanes & bit) == 0
                fresh = list(tiles)
                for k in range(8):
                    if k & bit == 0:
                        a, b = tiles[k], tiles[k | bit]
                        fresh[k] = jnp.where(clear, a, pltpu.roll(b, 16 * bit, 1))
                        fresh[k | bit] = jnp.where(clear, pltpu.roll(a, 128 - 16 * bit, 1), b)
                tiles = fresh
            for k in range(8):
                v, part = 4 * m + k // 2, k % 2
                out_ref[v, :, pl.ds(256 * part + 128 * high, 128)] = tiles[k]

    drain_across(piece, landed, send1, recv1)
    for copy in to_r + to_l + list(to_p.values()):
        copy.wait_send()
    drain_across(outbuf, back, send2, recv2)


def body(projections, ctf_weight, orient, angle_table):
    dma = pltpu.SemaphoreType.DMA
    return pl.pallas_call(
        kernel,
        out_shape=jax.ShapeDtypeStruct((16, 16, 512), jnp.float32),
        in_specs=[
            pl.BlockSpec(memory_space=pltpu.SMEM),
            pl.BlockSpec(memory_space=pltpu.VMEM),
            pl.BlockSpec(memory_space=pltpu.VMEM),
            pl.BlockSpec(memory_space=pltpu.VMEM),
        ],
        out_specs=pl.BlockSpec(memory_space=pltpu.VMEM),
        scratch_shapes=[
            pltpu.VMEM((16, 32, 128), jnp.bfloat16),
            pltpu.VMEM((16, 32, 128), jnp.bfloat16),
            pltpu.VMEM((64, 64, 256), jnp.bfloat16),
            pltpu.VMEM((768, 256), jnp.float32),
            pltpu.VMEM((16, 16, 512), jnp.bfloat16),
            pltpu.VMEM((16, 16, 512), jnp.bfloat16),
            dma((16,)), dma((16,)),
            dma((4,)), dma((4,)), dma((3,)), dma((3,)), dma((8,)), dma((8,)),
            dma((16,)), dma((16,)),
        ],
        compiler_params=pltpu.CompilerParams(
            collective_id=0, has_side_effects=True, vmem_limit_bytes=48 * 1024 * 1024
        ),
    )(orient, projections, ctf_weight, angle_table)


def solution(mesh):
    placed = (
        P(("rep", "pix"), "slab", None),
        P(("rep", "pix"), "slab", None),
        P(("rep", "pix")),
        P(),
    )
    return jax.shard_map(
        body, mesh=mesh, in_specs=placed, out_specs=P(("rep", "pix"), "slab", None), check_vma=False
    )
```

```python
import jax
import jax.numpy as jnp
from jax import lax
from jax.experimental import pallas as pl
from jax.experimental.pallas import tpu as pltpu
from jax.sharding import PartitionSpec as P

MESH = pl.DeviceIdType.MESH
RING = 8
FAR = 14


def slot_r(t):
    return 2 + 4 * (t - 1)


def slot_l(t):
    return 3 + 4 * (t - 1)


def slot_pr(t):
    return 4 + 4 * (t - 1)


def slot_pl(t):
    return 5 + 4 * (t - 1)


def kernel(
    orient_hbm, proj_hbm, ctf_hbm, table_hbm, out_ref,
    orient_ref, proj_ref, ctf_ref, table_ref, stage, piece, landed, gath, acc, outbuf, back,
    send1, recv1, send_r, recv_r, send_l, recv_l, send_p, recv_p, send2, recv2,
):
    staged = [
        pltpu.make_async_copy(src, dst, stage.at[k])
        for k, (src, dst) in enumerate(
            ((orient_hbm, orient_ref), (proj_hbm, proj_ref), (ctf_hbm, ctf_ref), (table_hbm, table_ref))
        )
    ]
    for copy in staged:
        copy.start()
    rep = lax.axis_index("rep")
    slab = lax.axis_index("slab")
    pix = lax.axis_index("pix")
    xc, core = rep // 2, rep % 2
    yc, zl = slab // 4, slab % 4
    zpos = pix * 4 + zl
    me = xc * 4 + yc
    sub = core * 2 + pix

    def plane(q):
        return ((q // 4) * 2 + core, (q % 4) * 4 + zl, pix)

    def along_z(step):
        z = (zpos + step + RING) % RING
        return (rep, yc * 4 + z % 4, z // 4)

    right, left = along_z(1), along_z(-1)
    partner = (xc * 2 + 1 - core, slab, pix)

    barrier = pltpu.get_barrier_semaphore()

    def greet(k, carry):
        pl.semaphore_signal(
            barrier, inc=1, device_id=plane((me + k) % 16), device_id_type=MESH
        )
        return carry

    lax.fori_loop(1, 16, greet, 0)
    for peer in (right, left, partner):
        pl.semaphore_signal(barrier, inc=1, device_id=peer, device_id_type=MESH)

    acc[...] = jnp.zeros_like(acc)
    for copy in staged:
        copy.wait()

    samples = proj_ref[...].reshape(64, 512).astype(jnp.float32)
    weights = ctf_ref[...].reshape(64, 256).astype(jnp.float32)
    real, imag = samples[:, :256], samples[:, 256:]
    first = jnp.concatenate([real, weights], axis=0).T
    second = jnp.concatenate([imag, imag], axis=0).T

    column = lax.broadcasted_iota(jnp.int32, (256, 128), 0)
    lane = lax.broadcasted_iota(jnp.int32, (256, 128), 1)
    geometry = jnp.zeros((4, 128), jnp.float32)
    for n in range(4):
        row = table_ref[orient_ref[n]].astype(jnp.float32).astype(jnp.bfloat16)
        pick = (column == slab * 16 + lane % 16) & ((lane // 16) % 4 == n)
        geometry += jnp.dot(
            row, pick.astype(jnp.float32).astype(jnp.bfloat16), preferred_element_type=jnp.float32
        )
    fx, fz = geometry[1:2] / 256.0, geometry[3:4] / 256.0
    facts = jnp.concatenate(
        [
            geometry[0:1],
            geometry[2:3],
            (1.0 - fx) * (1.0 - fz),
            (1.0 - fx) * fz,
            fx * (1.0 - fz),
            fx * fz,
            jnp.zeros((10, 128), jnp.float32),
        ],
        axis=0,
    )
    low_half = lax.broadcasted_iota(jnp.int32, (16, 128), 1) < 64
    for q in range(16):
        piece[q, 0:16, :] = first[16 * q : 16 * q + 16].astype(jnp.bfloat16)
        piece[q, 16:32, :] = jnp.where(
            low_half, second[16 * q : 16 * q + 16], facts
        ).astype(jnp.bfloat16)

    pl.semaphore_wait(barrier, 18)

    def across(src, dst, send, recv, k, into):
        to = (me + k) % 16
        return pltpu.make_async_remote_copy(
            src_ref=src.at[to], dst_ref=dst.at[into], send_sem=send.at[to], recv_sem=recv.at[into],
            device_id=plane(to), device_id_type=MESH,
        )

    def start_across(*refs):
        def go(k, carry):
            across(*refs, k, me).start()
            return carry

        lax.fori_loop(1, 16, go, 0)

    def land_across(*refs):
        def go(k, carry):
            across(*refs, k, (me - k + 16) % 16).wait_recv()
            return carry

        lax.fori_loop(1, 16, go, 0)

    def drain_across(*refs):
        def go(k, carry):
            across(*refs, k, me).wait_send()
            return carry

        lax.fori_loop(1, 16, go, 0)

    start_across(piece, landed, send1, recv1)
    landed[me] = piece[me]
    land_across(piece, landed, send1, recv1)

    half = lax.broadcasted_iota(jnp.int32, (32, 128), 1) < 64
    for j in range(8):
        a = landed[2 * j].astype(jnp.float32)
        b = landed[2 * j + 1].astype(jnp.float32)
        top = jnp.where(half, a, pltpu.roll(b, 64, 1)).astype(jnp.bfloat16)
        bottom = jnp.where(half, pltpu.roll(a, 64, 1), b).astype(jnp.bfloat16)
        at = pl.ds(128 * (j % 2), 128)
        gath[j // 2, 0:32, at] = top
        gath[j // 2, 32:64, at] = bottom

    def move(src, dst, part, send, recv, to):
        return pltpu.make_async_remote_copy(
            src_ref=gath.at[pl.ds(4 * src + 2 * part, 2)], dst_ref=gath.at[pl.ds(4 * dst + 2 * part, 2)],
            send_sem=send, recv_sem=recv, device_id=to, device_id_type=MESH,
        )

    def ringed(side, t, part):
        slot, send, recv, to = (
            (slot_r, send_r, recv_r, right) if side == "r" else (slot_l, send_l, recv_l, left)
        )
        src = 0 if t == 1 else slot(t - 1)
        k = 2 * (t - 1) + part
        return move(src, FAR if t == 4 else slot(t), part, send.at[k], recv.at[k], to)

    def shared(side, t, part):
        if t == 0:
            src, dst, k = 0, 1, 0
        elif t == 4:
            src, dst, k = FAR, FAR + 1, 7
        else:
            src, dst = (slot_r(t), slot_pr(t)) if side == "r" else (slot_l(t), slot_pl(t))
            k = 2 * t - (1 if side == "r" else 0)
        return move(src, dst, part, send_p.at[2 * k + part], recv_p.at[2 * k + part], partner)

    started = []

    def start(copy):
        copy.start()
        started.append(copy)

    def arrive(t, part):
        for side in ("r", "l"):
            if t == 4 and part != (0 if side == "r" else 1):
                continue
            ringed(side, t, part).wait_recv()
            if t < 3 or (t == 3 and part == (0 if side == "r" else 1)):
                start(ringed(side, t + 1, part))
            start(shared(side, t, part))

    row16 = lax.broadcasted_iota(jnp.int32, (16, 256), 0).astype(jnp.float32)

    def operands(g):
        block = gath[g]
        facts = block[48:64].astype(jnp.float32)
        x0 = facts[0:1].astype(jnp.int32)
        z0 = facts[1:2].astype(jnp.int32)

        def spread(v):
            return jnp.broadcast_to(v, (16, 256)).astype(jnp.bfloat16)

        zero = jnp.zeros((16, 256), jnp.bfloat16)
        pairs = []
        for i in range(2):
            xr = x0 + i
            x_ok = ((xr >> 4) & 3) == sub
            x_low = spread((xr & 15).astype(jnp.float32))
            keys, shares = [], []
            for j in range(2):
                zr = z0 + j
                ok = x_ok & (((zr >> 4) & 3) == zl)
                key = jnp.where(ok, (xr >> 6) * 64 + (zr >> 6) * 16 + (zr & 15), -1)
                keys.append(spread(key.astype(jnp.float32)))
                shares.append(spread(facts[2 + 2 * i + j : 3 + 2 * i + j]))
            right_side = []
            for t in range(16):
                here = (row16 + 16.0 * t).astype(jnp.bfloat16)
                right_side.append(
                    jnp.where(keys[0] == here, shares[0], jnp.where(keys[1] == here, shares[1], zero))
                )
            left_side = []
            for v in range(16):
                hit = x_low == jnp.full((16, 256), v, jnp.bfloat16)
                for c in range(3):
                    left_side.append(jnp.where(hit, block[16 * c : 16 * c + 16], zero))
            pairs.append((left_side, jnp.concatenate(right_side, axis=0)))
        return pairs

    def nt(a, b):
        return lax.dot_general(a, b, (((1,), (1,)), ((), ())), preferred_element_type=jnp.float32)

    def block_step(b, carry):
        pairs = []
        for e in range(4):
            pairs += operands(4 * b + e)
        size = 48 // 2
        for h in range(2):
            total = None
            for left_side, right_side in pairs:
                part = nt(jnp.concatenate(left_side[size * h : size * h + size], axis=0), right_side)
                total = part if total is None else total + part
            acc[pl.ds(16 * size * h, 16 * size), :] += total
        return carry

    def compute(first_slot, count):
        lax.fori_loop(first_slot, first_slot + count, block_step, 0)

    for part in range(2):
        start(ringed("r", 1, part))
        start(ringed("l", 1, part))
        start(shared("r", 0, part))
    compute(0, 1)
    for part in range(2):
        shared("r", 0, part).wait_recv()
    compute(1, 1)

    def shared_block(t):
        for part in range(2):
            shared("r", t, part).wait_recv()
            shared("l", t, part).wait_recv()
        compute(slot_pr(t), 2)

    for t in range(1, 4):
        arrive(t, 0)
        if t > 1:
            shared_block(t - 1)
        arrive(t, 1)
        compute(slot_r(t), 2)
    arrive(4, 0)
    shared_block(3)
    arrive(4, 1)
    compute(FAR, 1)
    for part in range(2):
        shared("r", 4, part).wait_recv()
    compute(FAR + 1, 1)

    rows = []
    for v in range(16):
        base = 48 * v
        bottom = acc[pl.ds(base + 32, 16), :] + 1.0
        rows.append(acc[pl.ds(base, 16), :] / bottom)
        rows.append(acc[pl.ds(base + 16, 16), :] / bottom)
    for m in range(4):
        turned = jnp.concatenate(rows[8 * m : 8 * m + 8], axis=0).T
        for o in range(16):
            outbuf[o, :, pl.ds(128 * m, 128)] = turned[16 * o : 16 * o + 16].astype(jnp.bfloat16)

    start_across(outbuf, back, send2, recv2)
    back[me] = outbuf[me]
    land_across(outbuf, back, send2, recv2)

    lanes = lax.broadcasted_iota(jnp.int32, (16, 128), 1) // 16
    for m in range(4):
        for high in range(2):
            tiles = [back[8 * high + k, :, pl.ds(128 * m, 128)].astype(jnp.float32) for k in range(8)]
            for bit in (1, 2, 4):
                clear = (lanes & bit) == 0
                fresh = list(tiles)
                for k in range(8):
                    if k & bit == 0:
                        a, b = tiles[k], tiles[k | bit]
                        fresh[k] = jnp.where(clear, a, pltpu.roll(b, 16 * bit, 1))
                        fresh[k | bit] = jnp.where(clear, pltpu.roll(a, 128 - 16 * bit, 1), b)
                tiles = fresh
            for k in range(8):
                v, part = 4 * m + k // 2, k % 2
                out_ref[v, :, pl.ds(256 * part + 128 * high, 128)] = tiles[k]

    drain_across(piece, landed, send1, recv1)
    for copy in started:
        copy.wait_send()
    drain_across(outbuf, back, send2, recv2)


def body(projections, ctf_weight, orient, angle_table):
    dma = pltpu.SemaphoreType.DMA
    return pl.pallas_call(
        kernel,
        out_shape=jax.ShapeDtypeStruct((16, 16, 512), jnp.float32),
        in_specs=[pl.BlockSpec(memory_space=pltpu.HBM)] * 4,
        out_specs=pl.BlockSpec(memory_space=pltpu.VMEM),
        scratch_shapes=[
            pltpu.SMEM((4,), jnp.int32),
            pltpu.VMEM((4, 16, 512), jnp.bfloat16),
            pltpu.VMEM((4, 16, 256), jnp.bfloat16),
            pltpu.VMEM((64, 4, 256), jnp.int32),
            dma((4,)),
            pltpu.VMEM((16, 32, 128), jnp.bfloat16),
            pltpu.VMEM((16, 32, 128), jnp.bfloat16),
            pltpu.VMEM((64, 64, 256), jnp.bfloat16),
            pltpu.VMEM((768, 256), jnp.float32),
            pltpu.VMEM((16, 16, 512), jnp.bfloat16),
            pltpu.VMEM((16, 16, 512), jnp.bfloat16),
            dma((16,)), dma((16,)),
            dma((8,)), dma((8,)), dma((8,)), dma((8,)), dma((16,)), dma((16,)),
            dma((16,)), dma((16,)),
        ],
        compiler_params=pltpu.CompilerParams(
            collective_id=0, has_side_effects=True, vmem_limit_bytes=48 * 1024 * 1024
        ),
    )(orient, projections, ctf_weight, angle_table)


def solution(mesh):
    placed = (
        P(("rep", "pix"), "slab", None),
        P(("rep", "pix"), "slab", None),
        P(("rep", "pix")),
        P(),
    )
    return jax.shard_map(
        body, mesh=mesh, in_specs=placed, out_specs=P(("rep", "pix"), "slab", None), check_vma=False
    )
```

```python
import jax
import jax.numpy as jnp
from jax import lax
from jax.experimental import pallas as pl
from jax.experimental.pallas import tpu as pltpu
from jax.sharding import PartitionSpec as P

MESH = pl.DeviceIdType.MESH
RING = 8
FAR = 14
HALVES = ((0, 112), (112, 96))


def slot_of(side, t):
    return 2 + 4 * (t - 1) + side


def slot_shared(side, t):
    return 4 + 4 * (t - 1) + side


def kernel(
    orient_hbm, proj_hbm, ctf_hbm, table_hbm, out_ref,
    orient_ref, proj_ref, ctf_ref, table_ref, stage, piece, landed, gath, acc, outbuf, back,
    send1, recv1, send_z, recv_z, send_p, recv_p, send2, recv2,
):
    staged = [
        pltpu.make_async_copy(src, dst, stage.at[k])
        for k, (src, dst) in enumerate(
            ((orient_hbm, orient_ref), (proj_hbm, proj_ref), (ctf_hbm, ctf_ref), (table_hbm, table_ref))
        )
    ]
    for copy in staged:
        copy.start()
    rep = lax.axis_index("rep")
    slab = lax.axis_index("slab")
    pix = lax.axis_index("pix")
    xc, core = rep // 2, rep % 2
    yc, zl = slab // 4, slab % 4
    zpos = pix * 4 + zl
    me = xc * 4 + yc
    sub = core * 2 + pix

    def plane(q):
        return ((q // 4) * 2 + core, (q % 4) * 4 + zl, pix)

    def along_z(step):
        z = (zpos + step + RING) % RING
        return (rep, yc * 4 + z % 4, z // 4)

    partner = (xc * 2 + 1 - core, slab, pix)

    barrier = pltpu.get_barrier_semaphore()

    def greet(k, carry):
        pl.semaphore_signal(
            barrier, inc=1, device_id=plane((me + k) % 16), device_id_type=MESH
        )
        return carry

    lax.fori_loop(1, 16, greet, 0)
    for peer in (along_z(1), along_z(-1), along_z(2), along_z(-2), partner):
        pl.semaphore_signal(barrier, inc=1, device_id=peer, device_id_type=MESH)

    acc[...] = jnp.zeros_like(acc)
    for copy in staged:
        copy.wait()

    samples = proj_ref[...].reshape(64, 512).astype(jnp.float32)
    weights = ctf_ref[...].reshape(64, 256).astype(jnp.float32)
    real, imag = samples[:, :256], samples[:, 256:]
    first = jnp.concatenate([real, weights], axis=0).T
    second = jnp.concatenate([imag, imag], axis=0).T

    column = lax.broadcasted_iota(jnp.int32, (256, 128), 0)
    lane = lax.broadcasted_iota(jnp.int32, (256, 128), 1)
    geometry = jnp.zeros((4, 128), jnp.float32)
    for n in range(4):
        row = table_ref[orient_ref[n]].astype(jnp.float32).astype(jnp.bfloat16)
        pick = (column == slab * 16 + lane % 16) & ((lane // 16) % 4 == n)
        geometry += jnp.dot(
            row, pick.astype(jnp.float32).astype(jnp.bfloat16), preferred_element_type=jnp.float32
        )
    facts = jnp.concatenate(
        [
            geometry[0:1], geometry[2:3], geometry[1:2], geometry[3:4],
            jnp.zeros((12, 128), jnp.float32),
        ],
        axis=0,
    )
    low_half = lax.broadcasted_iota(jnp.int32, (16, 128), 1) < 64
    for q in range(16):
        piece[q, 0:16, :] = first[16 * q : 16 * q + 16].astype(jnp.bfloat16)
        piece[q, 16:32, :] = jnp.where(
            low_half, second[16 * q : 16 * q + 16], facts
        ).astype(jnp.bfloat16)

    pl.semaphore_wait(barrier, 20)

    def across(src, dst, send, recv, k, into):
        to = (me + k) % 16
        return pltpu.make_async_remote_copy(
            src_ref=src.at[to], dst_ref=dst.at[into], send_sem=send.at[to], recv_sem=recv.at[into],
            device_id=plane(to), device_id_type=MESH,
        )

    def start_across(*refs):
        def go(k, carry):
            across(*refs, k, me).start()
            return carry

        lax.fori_loop(1, 16, go, 0)

    def land_across(*refs):
        def go(k, carry):
            across(*refs, k, (me - k + 16) % 16).wait_recv()
            return carry

        lax.fori_loop(1, 16, go, 0)

    def drain_across(*refs):
        def go(k, carry):
            across(*refs, k, me).wait_send()
            return carry

        lax.fori_loop(1, 16, go, 0)

    start_across(piece, landed, send1, recv1)
    landed[me] = piece[me]
    land_across(piece, landed, send1, recv1)

    half = lax.broadcasted_iota(jnp.int32, (32, 128), 1) < 64
    tables = []
    for j in range(8):
        a = landed[2 * j].astype(jnp.float32)
        b = landed[2 * j + 1].astype(jnp.float32)
        top = jnp.where(half, a, pltpu.roll(b, 64, 1)).astype(jnp.bfloat16)
        bottom = jnp.where(half, pltpu.roll(a, 64, 1), b)
        at = pl.ds(128 * (j % 2), 128)
        row = 16 + 48 * (j // 2)
        gath[0, row : row + 32, at] = top
        gath[0, row + 32 : row + 48, at] = bottom[0:16].astype(jnp.bfloat16)
        tables.append(bottom[16:20])
    gath[0, 0:16, :] = jnp.concatenate(
        [
            jnp.concatenate([tables[2 * g][f : f + 1], tables[2 * g + 1][f : f + 1]], axis=1)
            for f in range(4)
            for g in range(4)
        ],
        axis=0,
    ).astype(jnp.bfloat16)

    def move(src, dst, rows, send, recv, to):
        at = pl.ds(rows[0], rows[1])
        return pltpu.make_async_remote_copy(
            src_ref=gath.at[src, at], dst_ref=gath.at[dst, at],
            send_sem=send, recv_sem=recv, device_id=to, device_id_type=MESH,
        )

    def ringed(side, t, part):
        src = 0 if t < 3 else slot_of(side, 2)
        dst = FAR if t == 4 else slot_of(side, t)
        k = 8 * side + 2 * (t - 1) + part
        reach = (1, 2, 1, 2)[t - 1]
        return move(
            src, dst, HALVES[part], send_z.at[k], recv_z.at[k], along_z(reach * (1 - 2 * side))
        )

    def shared(side, t, part):
        if t == 0:
            src, dst, k = 0, 1, 0
        elif t == 4:
            src, dst, k = FAR, FAR + 1, 7
        else:
            src, dst, k = slot_of(side, t), slot_shared(side, t), 2 * t - 1 + side
        k = 2 * k + part
        return move(src, dst, HALVES[part], send_p.at[k], recv_p.at[k], partner)

    def arrive(side, t):
        for part in range(2):
            ringed(side, t, part).wait_recv()
            if t == 2:
                ringed(side, 3, part).start()

                @pl.when(side == part)
                def _():
                    ringed(part, 4, part).start()

            shared(side, t, part).start()

    row16 = lax.broadcasted_iota(jnp.int32, (16, 256), 0).astype(jnp.float32)

    def operands(block, g, keys, lows, shares):
        def spread(v):
            return jnp.broadcast_to(v[g : g + 1], (16, 256)).astype(jnp.bfloat16)

        base = 16 + 48 * g
        zero = jnp.zeros((16, 256), jnp.bfloat16)
        pairs = []
        for i in range(2):
            x_low = spread(lows[i])
            key = [spread(keys[i][j]) for j in range(2)]
            share = [spread(shares[i][j]) for j in range(2)]
            right_side = []
            for t in range(16):
                here = (row16 + 16.0 * t).astype(jnp.bfloat16)
                right_side.append(
                    jnp.where(key[0] == here, share[0], jnp.where(key[1] == here, share[1], zero))
                )
            left_side = []
            for v in range(16):
                hit = x_low == jnp.full((16, 256), v, jnp.bfloat16)
                for c in range(3):
                    left_side.append(
                        jnp.where(hit, block[base + 16 * c : base + 16 * c + 16], zero)
                    )
            pairs.append((left_side, jnp.concatenate(right_side, axis=0)))
        return pairs

    def nt(a, b):
        return lax.dot_general(a, b, (((1,), (1,)), ((), ())), preferred_element_type=jnp.float32)

    def factors(slot):
        block = gath[slot]
        facts = block[0:16].astype(jnp.float32)
        x0, z0 = facts[0:4].astype(jnp.int32), facts[4:8].astype(jnp.int32)
        fx, fz = facts[8:12] / 256.0, facts[12:16] / 256.0
        keys, lows, shares = [], [], []
        for i in range(2):
            xr = x0 + i
            x_ok = ((xr >> 4) & 3) == sub
            lows.append((xr & 15).astype(jnp.float32))
            keys.append([])
            shares.append([])
            for j in range(2):
                zr = z0 + j
                ok = x_ok & (((zr >> 4) & 3) == zl)
                key = jnp.where(ok, (xr >> 6) * 64 + (zr >> 6) * 16 + (zr & 15), -1)
                keys[i].append(key.astype(jnp.float32))
                shares[i].append((fx if i else 1.0 - fx) * (fz if j else 1.0 - fz))
        pairs = []
        for g in range(4):
            pairs += operands(block, g, keys, lows, shares)
        return pairs

    def accumulate(*slots):
        pairs = []
        for slot in slots:
            pairs += factors(slot)
        for h in range(2):
            total = None
            for left_side, right_side in pairs:
                part = nt(jnp.concatenate(left_side[24 * h : 24 * h + 24], axis=0), right_side)
                total = part if total is None else total + part
            acc[pl.ds(384 * h, 384), :] += total

    near = jnp.where(zpos < 4, 1, 0)
    away = 1 - near

    for t in range(1, 3):
        for part in range(2):
            for side in range(2):
                ringed(side, t, part).start()
            if t == 1:
                shared(0, 0, part).start()

    def landed_shared(side, t):
        for part in range(2):
            shared(side, t, part).wait_recv()
        return {0: 1, 4: FAR + 1}[t] if t in (0, 4) else slot_shared(side, t)

    accumulate(0)
    accumulate(landed_shared(0, 0))
    arrive(near, 1)
    accumulate(slot_of(near, 1))
    arrive(away, 1)
    accumulate(landed_shared(near, 1), slot_of(away, 1))
    arrive(near, 2)
    accumulate(landed_shared(away, 1), slot_of(near, 2))
    arrive(away, 2)
    accumulate(landed_shared(near, 2), slot_of(away, 2))
    arrive(near, 3)
    accumulate(landed_shared(away, 2), slot_of(near, 3))
    arrive(away, 3)
    for side in range(2):
        ringed(side, 4, side).wait_recv()
        shared(0, 4, side).start()
    accumulate(landed_shared(near, 3), slot_of(away, 3))
    accumulate(landed_shared(away, 3), FAR)
    accumulate(landed_shared(0, 4))

    rows = []
    for v in range(16):
        base = 48 * v
        bottom = acc[pl.ds(base + 32, 16), :] + 1.0
        rows.append(acc[pl.ds(base, 16), :] / bottom)
        rows.append(acc[pl.ds(base + 16, 16), :] / bottom)
    for m in range(4):
        turned = jnp.concatenate(rows[8 * m : 8 * m + 8], axis=0).T
        for o in range(16):
            outbuf[o, :, pl.ds(128 * m, 128)] = turned[16 * o : 16 * o + 16].astype(jnp.bfloat16)

    start_across(outbuf, back, send2, recv2)
    back[me] = outbuf[me]
    land_across(outbuf, back, send2, recv2)

    lanes = lax.broadcasted_iota(jnp.int32, (16, 128), 1) // 16
    for m in range(4):
        for high in range(2):
            tiles = [back[8 * high + k, :, pl.ds(128 * m, 128)].astype(jnp.float32) for k in range(8)]
            for bit in (1, 2, 4):
                clear = (lanes & bit) == 0
                fresh = list(tiles)
                for k in range(8):
                    if k & bit == 0:
                        a, b = tiles[k], tiles[k | bit]
                        fresh[k] = jnp.where(clear, a, pltpu.roll(b, 16 * bit, 1))
                        fresh[k | bit] = jnp.where(clear, pltpu.roll(a, 128 - 16 * bit, 1), b)
                tiles = fresh
            for k in range(8):
                v, part = 4 * m + k // 2, k % 2
                out_ref[v, :, pl.ds(256 * part + 128 * high, 128)] = tiles[k]

    drain_across(piece, landed, send1, recv1)
    for side in range(2):
        for t in range(1, 4):
            for part in range(2):
                ringed(side, t, part).wait_send()
        ringed(side, 4, side).wait_send()
    for part in range(2):
        for side, t in ((0, 0), (0, 1), (1, 1), (0, 2), (1, 2), (0, 3), (1, 3), (0, 4)):
            shared(side, t, part).wait_send()
    drain_across(outbuf, back, send2, recv2)


def body(projections, ctf_weight, orient, angle_table):
    dma = pltpu.SemaphoreType.DMA
    return pl.pallas_call(
        kernel,
        out_shape=jax.ShapeDtypeStruct((16, 16, 512), jnp.float32),
        in_specs=[pl.BlockSpec(memory_space=pltpu.HBM)] * 4,
        out_specs=pl.BlockSpec(memory_space=pltpu.VMEM),
        scratch_shapes=[
            pltpu.SMEM((4,), jnp.int32),
            pltpu.VMEM((4, 16, 512), jnp.bfloat16),
            pltpu.VMEM((4, 16, 256), jnp.bfloat16),
            pltpu.VMEM((64, 4, 256), jnp.int32),
            dma((4,)),
            pltpu.VMEM((16, 32, 128), jnp.bfloat16),
            pltpu.VMEM((16, 32, 128), jnp.bfloat16),
            pltpu.VMEM((16, 208, 256), jnp.bfloat16),
            pltpu.VMEM((768, 256), jnp.float32),
            pltpu.VMEM((16, 16, 512), jnp.bfloat16),
            pltpu.VMEM((16, 16, 512), jnp.bfloat16),
            dma((16,)), dma((16,)),
            dma((16,)), dma((16,)), dma((16,)), dma((16,)),
            dma((16,)), dma((16,)),
        ],
        compiler_params=pltpu.CompilerParams(
            collective_id=0, has_side_effects=True, vmem_limit_bytes=67043328
        ),
    )(orient, projections, ctf_weight, angle_table)


def solution(mesh):
    placed = (
        P(("rep", "pix"), "slab", None),
        P(("rep", "pix"), "slab", None),
        P(("rep", "pix")),
        P(),
    )
    return jax.shard_map(
        body, mesh=mesh, in_specs=placed, out_specs=P(("rep", "pix"), "slab", None), check_vma=False
    )
```

```python
import jax
import jax.numpy as jnp
from jax import lax
from jax.experimental import pallas as pl
from jax.experimental.pallas import tpu as pltpu
from jax.sharding import PartitionSpec as P

MESH = pl.DeviceIdType.MESH
RING = 8
FAR = 14
HALVES = ((0, 112), (112, 96))


def slot_of(side, t):
    return 2 + 4 * (t - 1) + side


def slot_shared(side, t):
    return 4 + 4 * (t - 1) + side


def kernel(
    orient_hbm, proj_hbm, ctf_hbm, table_hbm, out_ref,
    orient_ref, proj_ref, ctf_ref, table_ref, stage, piece, landed, gath, acc, outbuf, back,
    send1, recv1, send_z, recv_z, send_p, recv_p, send2, recv2,
):
    staged = [
        pltpu.make_async_copy(src, dst, stage.at[k])
        for k, (src, dst) in enumerate(
            ((orient_hbm, orient_ref), (proj_hbm, proj_ref), (ctf_hbm, ctf_ref), (table_hbm, table_ref))
        )
    ]
    for copy in staged:
        copy.start()
    rep = lax.axis_index("rep")
    slab = lax.axis_index("slab")
    pix = lax.axis_index("pix")
    xc, core = rep // 2, rep % 2
    yc, zl = slab // 4, slab % 4
    zpos = pix * 4 + zl
    me = xc * 4 + yc
    sub = core * 2 + pix

    def plane(q):
        return ((q // 4) * 2 + core, (q % 4) * 4 + zl, pix)

    def along_z(step):
        z = (zpos + step + RING) % RING
        return (rep, yc * 4 + z % 4, z // 4)

    partner = (xc * 2 + 1 - core, slab, pix)

    barrier = pltpu.get_barrier_semaphore()

    def greet(k, carry):
        pl.semaphore_signal(
            barrier, inc=1, device_id=plane((me + k) % 16), device_id_type=MESH
        )
        return carry

    lax.fori_loop(1, 16, greet, 0)
    for peer in (along_z(1), along_z(-1), partner):
        pl.semaphore_signal(barrier, inc=1, device_id=peer, device_id_type=MESH)

    acc[...] = jnp.zeros_like(acc)
    for copy in staged:
        copy.wait()

    samples = proj_ref[...].reshape(64, 512).astype(jnp.float32)
    weights = ctf_ref[...].reshape(64, 256).astype(jnp.float32)
    real, imag = samples[:, :256], samples[:, 256:]
    first = jnp.concatenate([real, weights], axis=0).T
    second = jnp.concatenate([imag, imag], axis=0).T

    column = lax.broadcasted_iota(jnp.int32, (256, 128), 0)
    lane = lax.broadcasted_iota(jnp.int32, (256, 128), 1)
    geometry = jnp.zeros((4, 128), jnp.float32)
    for n in range(4):
        row = table_ref[orient_ref[n]].astype(jnp.float32).astype(jnp.bfloat16)
        pick = (column == slab * 16 + lane % 16) & ((lane // 16) % 4 == n)
        geometry += jnp.dot(
            row, pick.astype(jnp.float32).astype(jnp.bfloat16), preferred_element_type=jnp.float32
        )
    facts = jnp.concatenate(
        [
            geometry[0:1], geometry[2:3], geometry[1:2], geometry[3:4],
            jnp.zeros((12, 128), jnp.float32),
        ],
        axis=0,
    )
    low_half = lax.broadcasted_iota(jnp.int32, (16, 128), 1) < 64
    for q in range(16):
        piece[q, 0:16, :] = first[16 * q : 16 * q + 16].astype(jnp.bfloat16)
        piece[q, 16:32, :] = jnp.where(
            low_half, second[16 * q : 16 * q + 16], facts
        ).astype(jnp.bfloat16)

    pl.semaphore_wait(barrier, 18)

    def across(src, dst, send, recv, k, into):
        to = (me + k) % 16
        return pltpu.make_async_remote_copy(
            src_ref=src.at[to], dst_ref=dst.at[into], send_sem=send.at[to], recv_sem=recv.at[into],
            device_id=plane(to), device_id_type=MESH,
        )

    def start_across(*refs):
        def go(k, carry):
            across(*refs, k, me).start()
            return carry

        lax.fori_loop(1, 16, go, 0)

    def land_across(*refs):
        def go(k, carry):
            across(*refs, k, (me - k + 16) % 16).wait_recv()
            return carry

        lax.fori_loop(1, 16, go, 0)

    def drain_across(*refs):
        def go(k, carry):
            across(*refs, k, me).wait_send()
            return carry

        lax.fori_loop(1, 16, go, 0)

    start_across(piece, landed, send1, recv1)
    landed[me] = piece[me]
    land_across(piece, landed, send1, recv1)

    half = lax.broadcasted_iota(jnp.int32, (32, 128), 1) < 64
    tables = []
    for j in range(8):
        a = landed[2 * j].astype(jnp.float32)
        b = landed[2 * j + 1].astype(jnp.float32)
        top = jnp.where(half, a, pltpu.roll(b, 64, 1)).astype(jnp.bfloat16)
        bottom = jnp.where(half, pltpu.roll(a, 64, 1), b)
        at = pl.ds(128 * (j % 2), 128)
        row = 16 + 48 * (j // 2)
        gath[0, row : row + 32, at] = top
        gath[0, row + 32 : row + 48, at] = bottom[0:16].astype(jnp.bfloat16)
        tables.append(bottom[16:20])
    gath[0, 0:16, :] = jnp.concatenate(
        [
            jnp.concatenate([tables[2 * g][f : f + 1], tables[2 * g + 1][f : f + 1]], axis=1)
            for f in range(4)
            for g in range(4)
        ],
        axis=0,
    ).astype(jnp.bfloat16)

    def move(src, dst, rows, send, recv, to):
        at = pl.ds(rows[0], rows[1])
        return pltpu.make_async_remote_copy(
            src_ref=gath.at[src, at], dst_ref=gath.at[dst, at],
            send_sem=send, recv_sem=recv, device_id=to, device_id_type=MESH,
        )

    def ringed(side, t, part):
        src = 0 if t == 1 else slot_of(side, t - 1)
        dst = FAR if t == 4 else slot_of(side, t)
        k = 8 * side + 2 * (t - 1) + part
        return move(
            src, dst, HALVES[part], send_z.at[k], recv_z.at[k], along_z(1 - 2 * side)
        )

    def shared(side, t, part):
        if t == 0:
            src, dst, k = 0, 1, 0
        elif t == 4:
            src, dst, k = FAR, FAR + 1, 7
        else:
            src, dst, k = slot_of(side, t), slot_shared(side, t), 2 * t - 1 + side
        k = 2 * k + part
        return move(src, dst, HALVES[part], send_p.at[k], recv_p.at[k], partner)

    def arrive(side, t, part):
        ringed(side, t, part).wait_recv()
        if t < 3:
            ringed(side, t + 1, part).start()
        elif t == 3:

            @pl.when(side == part)
            def _():
                ringed(part, 4, part).start()

        shared(side, t, part).start()

    row16 = lax.broadcasted_iota(jnp.int32, (16, 256), 0).astype(jnp.float32)

    def operands(block, g, keys, lows, shares):
        def spread(v):
            return jnp.broadcast_to(v[g : g + 1], (16, 256)).astype(jnp.bfloat16)

        base = 16 + 48 * g
        zero = jnp.zeros((16, 256), jnp.bfloat16)
        pairs = []
        for i in range(2):
            x_low = spread(lows[i])
            key = [spread(keys[i][j]) for j in range(2)]
            share = [spread(shares[i][j]) for j in range(2)]
            right_side = []
            for t in range(16):
                here = (row16 + 16.0 * t).astype(jnp.bfloat16)
                right_side.append(
                    jnp.where(key[0] == here, share[0], jnp.where(key[1] == here, share[1], zero))
                )
            left_side = []
            for v in range(16):
                hit = x_low == jnp.full((16, 256), v, jnp.bfloat16)
                for c in range(3):
                    left_side.append(
                        jnp.where(hit, block[base + 16 * c : base + 16 * c + 16], zero)
                    )
            pairs.append((left_side, jnp.concatenate(right_side, axis=0)))
        return pairs

    def nt(a, b):
        return lax.dot_general(a, b, (((1,), (1,)), ((), ())), preferred_element_type=jnp.float32)

    def factors(slot):
        block = gath[slot]
        facts = block[0:16].astype(jnp.float32)
        x0, z0 = facts[0:4].astype(jnp.int32), facts[4:8].astype(jnp.int32)
        fx, fz = facts[8:12] / 256.0, facts[12:16] / 256.0
        keys, lows, shares = [], [], []
        for i in range(2):
            xr = x0 + i
            x_ok = ((xr >> 4) & 3) == sub
            lows.append((xr & 15).astype(jnp.float32))
            keys.append([])
            shares.append([])
            for j in range(2):
                zr = z0 + j
                ok = x_ok & (((zr >> 4) & 3) == zl)
                key = jnp.where(ok, (xr >> 6) * 64 + (zr >> 6) * 16 + (zr & 15), -1)
                keys[i].append(key.astype(jnp.float32))
                shares[i].append((fx if i else 1.0 - fx) * (fz if j else 1.0 - fz))
        pairs = []
        for g in range(4):
            pairs += operands(block, g, keys, lows, shares)
        return pairs

    def accumulate(*slots):
        pairs = []
        for slot in slots:
            pairs += factors(slot)
        for h in range(2):
            total = None
            for left_side, right_side in pairs:
                part = nt(jnp.concatenate(left_side[24 * h : 24 * h + 24], axis=0), right_side)
                total = part if total is None else total + part
            acc[pl.ds(384 * h, 384), :] += total

    near = jnp.where(zpos < 4, 1, 0)
    away = 1 - near

    for part in range(2):
        for side in range(2):
            ringed(side, 1, part).start()
        shared(0, 0, part).start()

    def landed_shared(side, t):
        for part in range(2):
            shared(side, t, part).wait_recv()
        return {0: 1, 4: FAR + 1}[t] if t in (0, 4) else slot_shared(side, t)

    accumulate(0)
    accumulate(landed_shared(0, 0))
    arrive(near, 1, 0)
    arrive(near, 1, 1)
    accumulate(slot_of(near, 1))
    arrive(away, 1, 0)
    arrive(away, 1, 1)
    accumulate(slot_of(away, 1))
    accumulate(landed_shared(near, 1))
    arrive(near, 2, 0)
    arrive(away, 2, 0)
    accumulate(landed_shared(away, 1))
    arrive(near, 2, 1)
    arrive(away, 2, 1)
    accumulate(slot_of(near, 2))
    accumulate(slot_of(away, 2))
    arrive(near, 3, 0)
    accumulate(landed_shared(near, 2))
    arrive(near, 3, 1)
    accumulate(slot_of(near, 3))
    arrive(away, 3, 0)
    accumulate(landed_shared(away, 2))
    arrive(away, 3, 1)
    accumulate(slot_of(away, 3))
    accumulate(landed_shared(near, 3))
    arrive(0, 4, 0)
    accumulate(landed_shared(away, 3))
    arrive(1, 4, 1)
    accumulate(FAR)
    accumulate(landed_shared(0, 4))

    rows = []
    for v in range(16):
        base = 48 * v
        bottom = acc[pl.ds(base + 32, 16), :] + 1.0
        rows.append(acc[pl.ds(base, 16), :] / bottom)
        rows.append(acc[pl.ds(base + 16, 16), :] / bottom)
    for m in range(4):
        turned = jnp.concatenate(rows[8 * m : 8 * m + 8], axis=0).T
        for o in range(16):
            outbuf[o, :, pl.ds(128 * m, 128)] = turned[16 * o : 16 * o + 16].astype(jnp.bfloat16)

    start_across(outbuf, back, send2, recv2)
    back[me] = outbuf[me]
    land_across(outbuf, back, send2, recv2)

    lanes = lax.broadcasted_iota(jnp.int32, (16, 128), 1) // 16
    for m in range(4):
        for high in range(2):
            tiles = [back[8 * high + k, :, pl.ds(128 * m, 128)].astype(jnp.float32) for k in range(8)]
            for bit in (1, 2, 4):
                clear = (lanes & bit) == 0
                fresh = list(tiles)
                for k in range(8):
                    if k & bit == 0:
                        a, b = tiles[k], tiles[k | bit]
                        fresh[k] = jnp.where(clear, a, pltpu.roll(b, 16 * bit, 1))
                        fresh[k | bit] = jnp.where(clear, pltpu.roll(a, 128 - 16 * bit, 1), b)
                tiles = fresh
            for k in range(8):
                v, part = 4 * m + k // 2, k % 2
                out_ref[v, :, pl.ds(256 * part + 128 * high, 128)] = tiles[k]

    drain_across(piece, landed, send1, recv1)
    for side in range(2):
        for t in range(1, 4):
            for part in range(2):
                ringed(side, t, part).wait_send()
        ringed(side, 4, side).wait_send()
    for part in range(2):
        for side, t in ((0, 0), (0, 1), (1, 1), (0, 2), (1, 2), (0, 3), (1, 3), (0, 4)):
            shared(side, t, part).wait_send()
    drain_across(outbuf, back, send2, recv2)


def body(projections, ctf_weight, orient, angle_table):
    dma = pltpu.SemaphoreType.DMA
    return pl.pallas_call(
        kernel,
        out_shape=jax.ShapeDtypeStruct((16, 16, 512), jnp.float32),
        in_specs=[pl.BlockSpec(memory_space=pltpu.HBM)] * 4,
        out_specs=pl.BlockSpec(memory_space=pltpu.VMEM),
        scratch_shapes=[
            pltpu.SMEM((4,), jnp.int32),
            pltpu.VMEM((4, 16, 512), jnp.bfloat16),
            pltpu.VMEM((4, 16, 256), jnp.bfloat16),
            pltpu.VMEM((64, 4, 256), jnp.int32),
            dma((4,)),
            pltpu.VMEM((16, 32, 128), jnp.bfloat16),
            pltpu.VMEM((16, 32, 128), jnp.bfloat16),
            pltpu.VMEM((16, 208, 256), jnp.bfloat16),
            pltpu.VMEM((768, 256), jnp.float32),
            pltpu.VMEM((16, 16, 512), jnp.bfloat16),
            pltpu.VMEM((16, 16, 512), jnp.bfloat16),
            dma((16,)), dma((16,)),
            dma((16,)), dma((16,)), dma((16,)), dma((16,)),
            dma((16,)), dma((16,)),
        ],
        compiler_params=pltpu.CompilerParams(
            collective_id=0, has_side_effects=True, vmem_limit_bytes=67043328
        ),
    )(orient, projections, ctf_weight, angle_table)


def solution(mesh):
    placed = (
        P(("rep", "pix"), "slab", None),
        P(("rep", "pix"), "slab", None),
        P(("rep", "pix")),
        P(),
    )
    return jax.shard_map(
        body, mesh=mesh, in_specs=placed, out_specs=P(("rep", "pix"), "slab", None), check_vma=False
    )
```

```python
import jax
import jax.numpy as jnp
from jax import lax
from jax.experimental import pallas as pl
from jax.experimental.pallas import tpu as pltpu
from jax.sharding import PartitionSpec as P

MESH = pl.DeviceIdType.MESH
RING = 8
FAR = 14
HALVES = ((0, 112), (112, 96))


def slot_of(side, t):
    return 2 + 4 * (t - 1) + 2 * side


def kernel(
    orient_hbm, proj_hbm, ctf_hbm, table_hbm, out_ref,
    orient_ref, proj_ref, ctf_ref, table_ref, stage, piece, landed, gath, acc, outbuf, back,
    send1, recv1, send_z, recv_z, send_p, send_o, recv_o, send2, recv2,
):
    staged = [
        pltpu.make_async_copy(src, dst, stage.at[k])
        for k, (src, dst) in enumerate(
            ((orient_hbm, orient_ref), (proj_hbm, proj_ref), (ctf_hbm, ctf_ref), (table_hbm, table_ref))
        )
    ]
    for copy in staged:
        copy.start()
    rep = lax.axis_index("rep")
    slab = lax.axis_index("slab")
    pix = lax.axis_index("pix")
    xc, core = rep // 2, rep % 2
    yc, zl = slab // 4, slab % 4
    zpos = pix * 4 + zl
    me = xc * 4 + yc
    sub = core * 2 + pix
    hub = core == 1
    mine = 1 - core

    def plane(q):
        return ((q // 4) * 2 + core, (q % 4) * 4 + zl, pix)

    def along_z(step):
        z = (zpos + step + RING) % RING
        return (rep, yc * 4 + z % 4, z // 4)

    partner = (xc * 2 + 1 - core, slab, pix)

    barrier = pltpu.get_barrier_semaphore()

    def greet(k, carry):
        pl.semaphore_signal(
            barrier, inc=1, device_id=plane((me + k) % 16), device_id_type=MESH
        )
        return carry

    lax.fori_loop(1, 16, greet, 0)
    for peer in (along_z(1), along_z(-1), partner):
        pl.semaphore_signal(barrier, inc=1, device_id=peer, device_id_type=MESH)

    acc[...] = jnp.zeros_like(acc)
    for copy in staged:
        copy.wait()

    samples = proj_ref[...].reshape(64, 512).astype(jnp.float32)
    weights = ctf_ref[...].reshape(64, 256).astype(jnp.float32)
    real, imag = samples[:, :256], samples[:, 256:]
    first = jnp.concatenate([real, weights], axis=0).T
    second = jnp.concatenate([imag, imag], axis=0).T

    column = lax.broadcasted_iota(jnp.int32, (256, 128), 0)
    lane = lax.broadcasted_iota(jnp.int32, (256, 128), 1)
    geometry = jnp.zeros((4, 128), jnp.float32)
    for n in range(4):
        row = table_ref[orient_ref[n]].astype(jnp.float32).astype(jnp.bfloat16)
        pick = (column == slab * 16 + lane % 16) & ((lane // 16) % 4 == n)
        geometry += jnp.dot(
            row, pick.astype(jnp.float32).astype(jnp.bfloat16), preferred_element_type=jnp.float32
        )
    facts = jnp.concatenate(
        [
            geometry[0:1], geometry[2:3], geometry[1:2], geometry[3:4],
            jnp.zeros((12, 128), jnp.float32),
        ],
        axis=0,
    )
    low_half = lax.broadcasted_iota(jnp.int32, (16, 128), 1) < 64
    for q in range(16):
        piece[q, 0:16, :] = first[16 * q : 16 * q + 16].astype(jnp.bfloat16)
        piece[q, 16:32, :] = jnp.where(
            low_half, second[16 * q : 16 * q + 16], facts
        ).astype(jnp.bfloat16)

    pl.semaphore_wait(barrier, 18)

    def across(src, dst, send, recv, k, into):
        to = (me + k) % 16
        return pltpu.make_async_remote_copy(
            src_ref=src.at[to], dst_ref=dst.at[into], send_sem=send.at[to], recv_sem=recv.at[into],
            device_id=plane(to), device_id_type=MESH,
        )

    def start_across(*refs):
        def go(k, carry):
            across(*refs, k, me).start()
            return carry

        lax.fori_loop(1, 16, go, 0)

    def land_across(*refs):
        def go(k, carry):
            across(*refs, k, (me - k + 16) % 16).wait_recv()
            return carry

        lax.fori_loop(1, 16, go, 0)

    def drain_across(*refs):
        def go(k, carry):
            across(*refs, k, me).wait_send()
            return carry

        lax.fori_loop(1, 16, go, 0)

    start_across(piece, landed, send1, recv1)
    landed[me] = piece[me]
    land_across(piece, landed, send1, recv1)

    half = lax.broadcasted_iota(jnp.int32, (32, 128), 1) < 64
    tables = []
    for j in range(8):
        a = landed[2 * j].astype(jnp.float32)
        b = landed[2 * j + 1].astype(jnp.float32)
        top = jnp.where(half, a, pltpu.roll(b, 64, 1)).astype(jnp.bfloat16)
        bottom = jnp.where(half, pltpu.roll(a, 64, 1), b)
        at = pl.ds(128 * (j % 2), 128)
        row = 16 + 48 * (j // 2)
        gath[mine, row : row + 32, at] = top
        gath[mine, row + 32 : row + 48, at] = bottom[0:16].astype(jnp.bfloat16)
        tables.append(bottom[16:20])
    gath[mine, 0:16, :] = jnp.concatenate(
        [
            jnp.concatenate([tables[2 * g][f : f + 1], tables[2 * g + 1][f : f + 1]], axis=1)
            for f in range(4)
            for g in range(4)
        ],
        axis=0,
    ).astype(jnp.bfloat16)

    def move(src, dst, rows, send, recv, to):
        at = pl.ds(rows[0], rows[1])
        return pltpu.make_async_remote_copy(
            src_ref=gath.at[src, at], dst_ref=gath.at[dst, at],
            send_sem=send, recv_sem=recv, device_id=to, device_id_type=MESH,
        )

    def slots(side, t, part):
        return (FAR if t == 4 else slot_of(side, t)) + part // 2

    def index(side, t, part):
        return 16 * side + 4 * (t - 1) + part

    def ringed(side, t, part):
        src = part // 2 if t == 1 else slot_of(side, t - 1) + part // 2
        k = index(side, t, part)
        return move(
            src, slots(side, t, part), HALVES[part % 2], send_z.at[k], recv_z.at[k],
            along_z(1 - 2 * side),
        )

    def shared(side, t, part):
        slot, k = slots(side, t, part), index(side, t, part)
        return move(slot, slot, HALVES[part % 2], send_p.at[k], recv_z.at[k], partner)

    def exchanged(part):
        return move(mine, mine, HALVES[part], send_o.at[part], recv_o.at[part], partner)

    def arrive_partner(part):
        exchanged(part).wait_recv()

        @pl.when(hub)
        def _():
            for side in range(2):
                ringed(side, 1, 2 + part).start()

    def arrive(side, t, part):
        ringed(side, t, part).wait_recv()

        @pl.when(hub)
        def _():
            if t < 3:
                ringed(side, t + 1, part).start()
            shared(side, t, part).start()

        if t == 3:

            @pl.when(hub & (side == part % 2))
            def _():
                ringed(part % 2, 4, part).start()

    row16 = lax.broadcasted_iota(jnp.int32, (16, 256), 0).astype(jnp.float32)

    def operands(block, g, keys, lows, shares):
        def spread(v):
            return jnp.broadcast_to(v[g : g + 1], (16, 256)).astype(jnp.bfloat16)

        base = 16 + 48 * g
        zero = jnp.zeros((16, 256), jnp.bfloat16)
        pairs = []
        for i in range(2):
            x_low = spread(lows[i])
            key = [spread(keys[i][j]) for j in range(2)]
            share = [spread(shares[i][j]) for j in range(2)]
            right_side = []
            for t in range(16):
                here = (row16 + 16.0 * t).astype(jnp.bfloat16)
                right_side.append(
                    jnp.where(key[0] == here, share[0], jnp.where(key[1] == here, share[1], zero))
                )
            left_side = []
            for v in range(16):
                hit = x_low == jnp.full((16, 256), v, jnp.bfloat16)
                for c in range(3):
                    left_side.append(
                        jnp.where(hit, block[base + 16 * c : base + 16 * c + 16], zero)
                    )
            pairs.append((left_side, jnp.concatenate(right_side, axis=0)))
        return pairs

    def nt(a, b):
        return lax.dot_general(a, b, (((1,), (1,)), ((), ())), preferred_element_type=jnp.float32)

    def factors(slot):
        block = gath[slot]
        facts = block[0:16].astype(jnp.float32)
        x0, z0 = facts[0:4].astype(jnp.int32), facts[4:8].astype(jnp.int32)
        fx, fz = facts[8:12] / 256.0, facts[12:16] / 256.0
        keys, lows, shares = [], [], []
        for i in range(2):
            xr = x0 + i
            x_ok = ((xr >> 4) & 3) == sub
            lows.append((xr & 15).astype(jnp.float32))
            keys.append([])
            shares.append([])
            for j in range(2):
                zr = z0 + j
                ok = x_ok & (((zr >> 4) & 3) == zl)
                key = jnp.where(ok, (xr >> 6) * 64 + (zr >> 6) * 16 + (zr & 15), -1)
                keys[i].append(key.astype(jnp.float32))
                shares[i].append((fx if i else 1.0 - fx) * (fz if j else 1.0 - fz))
        pairs = []
        for g in range(4):
            pairs += operands(block, g, keys, lows, shares)
        return pairs

    def accumulate(*slots):
        pairs = []
        for slot in slots:
            pairs += factors(slot)
        for h in range(2):
            total = None
            for left_side, right_side in pairs:
                part = nt(jnp.concatenate(left_side[24 * h : 24 * h + 24], axis=0), right_side)
                total = part if total is None else total + part
            acc[pl.ds(384 * h, 384), :] += total

    near = jnp.where(zpos < 4, 1, 0)
    away = 1 - near

    @pl.when(hub)
    def _():
        for part in range(2):
            for side in range(2):
                ringed(side, 1, part).start()

    for part in range(2):
        exchanged(part).start()
    accumulate(mine)
    arrive_partner(0)
    arrive_partner(1)
    accumulate(core)
    arrive(near, 1, 0)
    arrive(near, 1, 1)
    accumulate(slot_of(near, 1))
    arrive(near, 1, 2)
    arrive(near, 1, 3)
    accumulate(slot_of(near, 1) + 1)
    arrive(away, 1, 0)
    arrive(away, 1, 1)
    accumulate(slot_of(away, 1))
    arrive(away, 1, 2)
    arrive(away, 1, 3)
    accumulate(slot_of(away, 1) + 1)
    arrive(near, 2, 0)
    arrive(away, 2, 0)
    arrive(near, 2, 1)
    arrive(away, 2, 1)
    accumulate(slot_of(near, 2))
    arrive(near, 2, 2)
    arrive(away, 2, 2)
    accumulate(slot_of(away, 2))
    arrive(near, 2, 3)
    arrive(away, 2, 3)
    arrive(near, 3, 0)
    accumulate(slot_of(near, 2) + 1)
    arrive(near, 3, 1)
    accumulate(slot_of(away, 2) + 1)
    arrive(near, 3, 2)
    accumulate(slot_of(near, 3))
    arrive(away, 3, 0)
    arrive(near, 3, 3)
    arrive(away, 3, 1)
    accumulate(slot_of(near, 3) + 1)
    arrive(away, 3, 2)
    arrive(away, 3, 3)
    accumulate(slot_of(away, 3))
    accumulate(slot_of(away, 3) + 1)
    arrive(0, 4, 0)
    arrive(1, 4, 1)
    accumulate(FAR)
    arrive(0, 4, 2)
    arrive(1, 4, 3)
    accumulate(FAR + 1)

    rows = []
    for v in range(16):
        base = 48 * v
        bottom = acc[pl.ds(base + 32, 16), :] + 1.0
        rows.append(acc[pl.ds(base, 16), :] / bottom)
        rows.append(acc[pl.ds(base + 16, 16), :] / bottom)
    for m in range(4):
        turned = jnp.concatenate(rows[8 * m : 8 * m + 8], axis=0).T
        for o in range(16):
            outbuf[o, :, pl.ds(128 * m, 128)] = turned[16 * o : 16 * o + 16].astype(jnp.bfloat16)

    start_across(outbuf, back, send2, recv2)
    back[me] = outbuf[me]
    land_across(outbuf, back, send2, recv2)

    lanes = lax.broadcasted_iota(jnp.int32, (16, 128), 1) // 16
    for m in range(4):
        for high in range(2):
            tiles = [back[8 * high + k, :, pl.ds(128 * m, 128)].astype(jnp.float32) for k in range(8)]
            for bit in (1, 2, 4):
                clear = (lanes & bit) == 0
                fresh = list(tiles)
                for k in range(8):
                    if k & bit == 0:
                        a, b = tiles[k], tiles[k | bit]
                        fresh[k] = jnp.where(clear, a, pltpu.roll(b, 16 * bit, 1))
                        fresh[k | bit] = jnp.where(clear, pltpu.roll(a, 128 - 16 * bit, 1), b)
                tiles = fresh
            for k in range(8):
                v, part = 4 * m + k // 2, k % 2
                out_ref[v, :, pl.ds(256 * part + 128 * high, 128)] = tiles[k].astype(jnp.bfloat16)

    drain_across(piece, landed, send1, recv1)
    for part in range(2):
        exchanged(part).wait_send()

    @pl.when(hub)
    def _():
        for side in range(2):
            for t in range(1, 5):
                for part in range(4) if t < 4 else (side, 2 + side):
                    ringed(side, t, part).wait_send()
                    shared(side, t, part).wait_send()

    drain_across(outbuf, back, send2, recv2)


def body(projections, ctf_weight, orient, angle_table):
    dma = pltpu.SemaphoreType.DMA
    return pl.pallas_call(
        kernel,
        out_shape=jax.ShapeDtypeStruct((16, 16, 512), jnp.bfloat16),
        in_specs=[pl.BlockSpec(memory_space=pltpu.HBM)] * 4,
        out_specs=pl.BlockSpec(memory_space=pltpu.VMEM),
        scratch_shapes=[
            pltpu.SMEM((4,), jnp.int32),
            pltpu.VMEM((4, 16, 512), jnp.bfloat16),
            pltpu.VMEM((4, 16, 256), jnp.bfloat16),
            pltpu.VMEM((64, 4, 256), jnp.int32),
            dma((4,)),
            pltpu.VMEM((16, 32, 128), jnp.bfloat16),
            pltpu.VMEM((16, 32, 128), jnp.bfloat16),
            pltpu.VMEM((16, 208, 256), jnp.bfloat16),
            pltpu.VMEM((768, 256), jnp.float32),
            pltpu.VMEM((16, 16, 512), jnp.bfloat16),
            pltpu.VMEM((16, 16, 512), jnp.bfloat16),
            dma((16,)), dma((16,)),
            dma((32,)), dma((32,)), dma((32,)), dma((2,)), dma((2,)),
            dma((16,)), dma((16,)),
        ],
        compiler_params=pltpu.CompilerParams(
            collective_id=0, has_side_effects=True, vmem_limit_bytes=67043328
        ),
    )(orient, projections, ctf_weight, angle_table).astype(jnp.float32)


def solution(mesh):
    placed = (
        P(("rep", "pix"), "slab", None),
        P(("rep", "pix"), "slab", None),
        P(("rep", "pix")),
        P(),
    )
    return jax.shard_map(
        body, mesh=mesh, in_specs=placed, out_specs=P(("rep", "pix"), "slab", None), check_vma=False
    )
```

```python
import jax
import jax.numpy as jnp
from jax import lax
from jax.experimental import pallas as pl
from jax.experimental.pallas import tpu as pltpu
from jax.sharding import PartitionSpec as P

MESH = pl.DeviceIdType.MESH
RING = 8
FAR = 14
FARTHEST_FIRST = (
    (2, 2), (2, 1), (2, 3), (1, 2), (3, 2), (1, 1), (1, 3), (3, 1), (3, 3),
    (2, 0), (0, 2), (1, 0), (3, 0), (0, 1), (0, 3),
)
HALVES = ((0, 112), (112, 96))


def slot_of(side, t):
    return 2 + 4 * (t - 1) + 2 * side


def kernel(
    orient_hbm, proj_hbm, ctf_hbm, table_hbm, out_ref,
    orient_ref, proj_ref, ctf_ref, table_ref, stage, piece, landed, gath, acc, outbuf, back,
    send1, recv1, send_z, recv_z, send_p, send_o, recv_o, send2, recv2,
):
    staged = [
        pltpu.make_async_copy(src, dst, stage.at[k])
        for k, (src, dst) in enumerate(
            ((orient_hbm, orient_ref), (proj_hbm, proj_ref), (ctf_hbm, ctf_ref), (table_hbm, table_ref))
        )
    ]
    for copy in staged:
        copy.start()
    rep = lax.axis_index("rep")
    slab = lax.axis_index("slab")
    pix = lax.axis_index("pix")
    xc, core = rep // 2, rep % 2
    yc, zl = slab // 4, slab % 4
    zpos = pix * 4 + zl
    me = xc * 4 + yc
    sub = core * 2 + pix
    hub = core == 1
    mine = 1 - core

    def plane(q):
        return ((q // 4) * 2 + core, (q % 4) * 4 + zl, pix)

    def along_z(step):
        z = (zpos + step + RING) % RING
        return (rep, yc * 4 + z % 4, z // 4)

    partner = (xc * 2 + 1 - core, slab, pix)

    barrier = pltpu.get_barrier_semaphore()

    def greet(k, carry):
        pl.semaphore_signal(
            barrier, inc=1, device_id=plane((me + k) % 16), device_id_type=MESH
        )
        return carry

    lax.fori_loop(1, 16, greet, 0)
    for peer in (along_z(1), along_z(-1), partner):
        pl.semaphore_signal(barrier, inc=1, device_id=peer, device_id_type=MESH)

    acc[...] = jnp.zeros_like(acc)
    for copy in staged:
        copy.wait()

    samples = proj_ref[...].reshape(64, 512).astype(jnp.float32)
    weights = ctf_ref[...].reshape(64, 256).astype(jnp.float32)
    real, imag = samples[:, :256], samples[:, 256:]
    first = jnp.concatenate([real, weights], axis=0).T
    second = jnp.concatenate([imag, imag], axis=0).T

    column = lax.broadcasted_iota(jnp.int32, (256, 128), 0)
    lane = lax.broadcasted_iota(jnp.int32, (256, 128), 1)
    geometry = jnp.zeros((4, 128), jnp.float32)
    for n in range(4):
        row = table_ref[orient_ref[n]].astype(jnp.float32).astype(jnp.bfloat16)
        pick = (column == slab * 16 + lane % 16) & ((lane // 16) % 4 == n)
        geometry += jnp.dot(
            row, pick.astype(jnp.float32).astype(jnp.bfloat16), preferred_element_type=jnp.float32
        )
    facts = jnp.concatenate(
        [
            geometry[0:1], geometry[2:3], geometry[1:2], geometry[3:4],
            jnp.zeros((12, 128), jnp.float32),
        ],
        axis=0,
    )
    low_half = lax.broadcasted_iota(jnp.int32, (16, 128), 1) < 64
    for q in range(16):
        piece[q, 0:16, :] = first[16 * q : 16 * q + 16].astype(jnp.bfloat16)
        piece[q, 16:32, :] = jnp.where(
            low_half, second[16 * q : 16 * q + 16], facts
        ).astype(jnp.bfloat16)

    pl.semaphore_wait(barrier, 18)

    def across(src, dst, send, recv, k, into):
        to = (me + k) % 16
        return pltpu.make_async_remote_copy(
            src_ref=src.at[to], dst_ref=dst.at[into], send_sem=send.at[to], recv_sem=recv.at[into],
            device_id=plane(to), device_id_type=MESH,
        )

    def start_across(src, dst, send, recv):
        for dx, dy in FARTHEST_FIRST:
            to = (xc + dx) % 4 * 4 + (yc + dy) % 4
            pltpu.make_async_remote_copy(
                src_ref=src.at[to], dst_ref=dst.at[me], send_sem=send.at[to], recv_sem=recv.at[me],
                device_id=plane(to), device_id_type=MESH,
            ).start()

    def land_across(*refs):
        def go(k, carry):
            across(*refs, k, (me - k + 16) % 16).wait_recv()
            return carry

        lax.fori_loop(1, 16, go, 0)

    def drain_across(*refs):
        def go(k, carry):
            across(*refs, k, me).wait_send()
            return carry

        lax.fori_loop(1, 16, go, 0)

    start_across(piece, landed, send1, recv1)
    landed[me] = piece[me]
    land_across(piece, landed, send1, recv1)

    half = lax.broadcasted_iota(jnp.int32, (32, 128), 1) < 64
    tables = []
    for j in range(8):
        a = landed[2 * j].astype(jnp.float32)
        b = landed[2 * j + 1].astype(jnp.float32)
        top = jnp.where(half, a, pltpu.roll(b, 64, 1)).astype(jnp.bfloat16)
        bottom = jnp.where(half, pltpu.roll(a, 64, 1), b)
        at = pl.ds(128 * (j % 2), 128)
        row = 16 + 48 * (j // 2)
        gath[mine, row : row + 32, at] = top
        gath[mine, row + 32 : row + 48, at] = bottom[0:16].astype(jnp.bfloat16)
        tables.append(bottom[16:20])
    gath[mine, 0:16, :] = jnp.concatenate(
        [
            jnp.concatenate([tables[2 * g][f : f + 1], tables[2 * g + 1][f : f + 1]], axis=1)
            for f in range(4)
            for g in range(4)
        ],
        axis=0,
    ).astype(jnp.bfloat16)

    def move(src, dst, rows, send, recv, to):
        at = pl.ds(rows[0], rows[1])
        return pltpu.make_async_remote_copy(
            src_ref=gath.at[src, at], dst_ref=gath.at[dst, at],
            send_sem=send, recv_sem=recv, device_id=to, device_id_type=MESH,
        )

    def slots(side, t, part):
        return (FAR if t == 4 else slot_of(side, t)) + part // 2

    def index(side, t, part):
        return 16 * side + 4 * (t - 1) + part

    def ringed(side, t, part):
        src = part // 2 if t == 1 else slot_of(side, t - 1) + part // 2
        k = index(side, t, part)
        return move(
            src, slots(side, t, part), HALVES[part % 2], send_z.at[k], recv_z.at[k],
            along_z(1 - 2 * side),
        )

    def shared(side, t, part):
        slot, k = slots(side, t, part), index(side, t, part)
        return move(slot, slot, HALVES[part % 2], send_p.at[k], recv_z.at[k], partner)

    def exchanged(part):
        return move(mine, mine, HALVES[part], send_o.at[part], recv_o.at[part], partner)

    def arrive_partner(part):
        exchanged(part).wait_recv()

        @pl.when(hub)
        def _():
            for side in range(2):
                ringed(side, 1, 2 + part).start()

    def arrive(side, t, part):
        ringed(side, t, part).wait_recv()

        @pl.when(hub)
        def _():
            if t < 3:
                ringed(side, t + 1, part).start()
            shared(side, t, part).start()

        if t == 3:

            @pl.when(hub & (side == part % 2))
            def _():
                ringed(part % 2, 4, part).start()

    row16 = lax.broadcasted_iota(jnp.int32, (16, 256), 0).astype(jnp.float32)

    def operands(block, g, keys, lows, shares):
        def spread(v):
            return jnp.broadcast_to(v[g : g + 1], (16, 256)).astype(jnp.bfloat16)

        base = 16 + 48 * g
        zero = jnp.zeros((16, 256), jnp.bfloat16)
        pairs = []
        for i in range(2):
            x_low = spread(lows[i])
            key = [spread(keys[i][j]) for j in range(2)]
            share = [spread(shares[i][j]) for j in range(2)]
            right_side = []
            for t in range(16):
                here = (row16 + 16.0 * t).astype(jnp.bfloat16)
                right_side.append(
                    jnp.where(key[0] == here, share[0], jnp.where(key[1] == here, share[1], zero))
                )
            left_side = []
            for v in range(16):
                hit = x_low == jnp.full((16, 256), v, jnp.bfloat16)
                for c in range(3):
                    left_side.append(
                        jnp.where(hit, block[base + 16 * c : base + 16 * c + 16], zero)
                    )
            pairs.append((left_side, jnp.concatenate(right_side, axis=0)))
        return pairs

    def nt(a, b):
        return lax.dot_general(a, b, (((1,), (1,)), ((), ())), preferred_element_type=jnp.float32)

    def factors(slot):
        block = gath[slot]
        facts = block[0:16].astype(jnp.float32)
        x0, z0 = facts[0:4].astype(jnp.int32), facts[4:8].astype(jnp.int32)
        fx, fz = facts[8:12] / 256.0, facts[12:16] / 256.0
        keys, lows, shares = [], [], []
        for i in range(2):
            xr = x0 + i
            x_ok = ((xr >> 4) & 3) == sub
            lows.append((xr & 15).astype(jnp.float32))
            keys.append([])
            shares.append([])
            for j in range(2):
                zr = z0 + j
                ok = x_ok & (((zr >> 4) & 3) == zl)
                key = jnp.where(ok, (xr >> 6) * 64 + (zr >> 6) * 16 + (zr & 15), -1)
                keys[i].append(key.astype(jnp.float32))
                shares[i].append((fx if i else 1.0 - fx) * (fz if j else 1.0 - fz))
        pairs = []
        for g in range(4):
            pairs += operands(block, g, keys, lows, shares)
        return pairs

    def accumulate(*slots):
        pairs = []
        for slot in slots:
            pairs += factors(slot)
        for h in range(2):
            total = None
            for left_side, right_side in pairs:
                part = nt(jnp.concatenate(left_side[24 * h : 24 * h + 24], axis=0), right_side)
                total = part if total is None else total + part
            acc[pl.ds(384 * h, 384), :] += total

    near = jnp.where(zpos < 4, 1, 0)
    away = 1 - near

    @pl.when(hub)
    def _():
        for part in range(2):
            for side in range(2):
                ringed(side, 1, part).start()

    for part in range(2):
        exchanged(part).start()
    accumulate(mine)
    arrive_partner(0)
    arrive_partner(1)
    accumulate(core)
    arrive(near, 1, 0)
    arrive(near, 1, 1)
    accumulate(slot_of(near, 1))
    arrive(near, 1, 2)
    arrive(near, 1, 3)
    accumulate(slot_of(near, 1) + 1)
    arrive(away, 1, 0)
    arrive(away, 1, 1)
    accumulate(slot_of(away, 1))
    arrive(away, 1, 2)
    arrive(away, 1, 3)
    accumulate(slot_of(away, 1) + 1)
    arrive(near, 2, 0)
    arrive(away, 2, 0)
    arrive(near, 2, 1)
    arrive(away, 2, 1)
    accumulate(slot_of(near, 2))
    arrive(near, 2, 2)
    arrive(away, 2, 2)
    accumulate(slot_of(away, 2))
    arrive(near, 2, 3)
    arrive(away, 2, 3)
    arrive(near, 3, 0)
    accumulate(slot_of(near, 2) + 1)
    arrive(near, 3, 1)
    accumulate(slot_of(away, 2) + 1)
    arrive(near, 3, 2)
    accumulate(slot_of(near, 3))
    arrive(away, 3, 0)
    arrive(near, 3, 3)
    arrive(away, 3, 1)
    accumulate(slot_of(near, 3) + 1)
    arrive(away, 3, 2)
    arrive(away, 3, 3)
    accumulate(slot_of(away, 3))
    accumulate(slot_of(away, 3) + 1)
    arrive(0, 4, 0)
    arrive(1, 4, 1)
    accumulate(FAR)
    arrive(0, 4, 2)
    arrive(1, 4, 3)
    accumulate(FAR + 1)

    rows = []
    for v in range(16):
        base = 48 * v
        bottom = acc[pl.ds(base + 32, 16), :] + 1.0
        rows.append(acc[pl.ds(base, 16), :] / bottom)
        rows.append(acc[pl.ds(base + 16, 16), :] / bottom)
    for m in range(4):
        turned = jnp.concatenate(rows[8 * m : 8 * m + 8], axis=0).T
        for o in range(16):
            outbuf[o, :, pl.ds(128 * m, 128)] = turned[16 * o : 16 * o + 16].astype(jnp.bfloat16)

    start_across(outbuf, back, send2, recv2)
    back[me] = outbuf[me]
    land_across(outbuf, back, send2, recv2)

    lanes = lax.broadcasted_iota(jnp.int32, (16, 128), 1) // 16
    for m in range(4):
        for high in range(2):
            tiles = [back[8 * high + k, :, pl.ds(128 * m, 128)].astype(jnp.float32) for k in range(8)]
            for bit in (1, 2, 4):
                clear = (lanes & bit) == 0
                fresh = list(tiles)
                for k in range(8):
                    if k & bit == 0:
                        a, b = tiles[k], tiles[k | bit]
                        fresh[k] = jnp.where(clear, a, pltpu.roll(b, 16 * bit, 1))
                        fresh[k | bit] = jnp.where(clear, pltpu.roll(a, 128 - 16 * bit, 1), b)
                tiles = fresh
            for k in range(8):
                v, part = 4 * m + k // 2, k % 2
                out_ref[v, :, pl.ds(256 * part + 128 * high, 128)] = tiles[k].astype(jnp.bfloat16)

    drain_across(piece, landed, send1, recv1)
    for part in range(2):
        exchanged(part).wait_send()

    @pl.when(hub)
    def _():
        for side in range(2):
            for t in range(1, 5):
                for part in range(4) if t < 4 else (side, 2 + side):
                    ringed(side, t, part).wait_send()
                    shared(side, t, part).wait_send()

    drain_across(outbuf, back, send2, recv2)


def body(projections, ctf_weight, orient, angle_table):
    dma = pltpu.SemaphoreType.DMA
    return pl.pallas_call(
        kernel,
        out_shape=jax.ShapeDtypeStruct((16, 16, 512), jnp.bfloat16),
        in_specs=[pl.BlockSpec(memory_space=pltpu.HBM)] * 4,
        out_specs=pl.BlockSpec(memory_space=pltpu.VMEM),
        scratch_shapes=[
            pltpu.SMEM((4,), jnp.int32),
            pltpu.VMEM((4, 16, 512), jnp.bfloat16),
            pltpu.VMEM((4, 16, 256), jnp.bfloat16),
            pltpu.VMEM((64, 4, 256), jnp.int32),
            dma((4,)),
            pltpu.VMEM((16, 32, 128), jnp.bfloat16),
            pltpu.VMEM((16, 32, 128), jnp.bfloat16),
            pltpu.VMEM((16, 208, 256), jnp.bfloat16),
            pltpu.VMEM((768, 256), jnp.float32),
            pltpu.VMEM((16, 16, 512), jnp.bfloat16),
            pltpu.VMEM((16, 16, 512), jnp.bfloat16),
            dma((16,)), dma((16,)),
            dma((32,)), dma((32,)), dma((32,)), dma((2,)), dma((2,)),
            dma((16,)), dma((16,)),
        ],
        compiler_params=pltpu.CompilerParams(
            collective_id=0, has_side_effects=True, vmem_limit_bytes=67043328
        ),
    )(orient, projections, ctf_weight, angle_table).astype(jnp.float32)


def solution(mesh):
    placed = (
        P(("rep", "pix"), "slab", None),
        P(("rep", "pix"), "slab", None),
        P(("rep", "pix")),
        P(),
    )
    return jax.shard_map(
        body, mesh=mesh, in_specs=placed, out_specs=P(("rep", "pix"), "slab", None), check_vma=False
    )
```

```python
import jax
import jax.numpy as jnp
from jax import lax
from jax.experimental import pallas as pl
from jax.experimental.pallas import tpu as pltpu
from jax.sharding import PartitionSpec as P

MESH = pl.DeviceIdType.MESH
RING = 8
FAR = 14
FARTHEST_FIRST = (
    (2, 2), (2, 1), (2, 3), (1, 2), (3, 2), (1, 1), (1, 3), (3, 1), (3, 3),
    (2, 0), (0, 2), (1, 0), (3, 0), (0, 1), (0, 3),
)
HALVES = ((0, 112), (112, 96))


def slot_of(side, t):
    return 2 + 4 * (t - 1) + 2 * side


def kernel(
    orient_hbm, proj_hbm, ctf_hbm, table_hbm, out_ref,
    orient_ref, proj_ref, ctf_ref, table_ref, stage, piece, landed, gath, acc, outbuf, back,
    send1, recv1, send_z, recv_z, send_p, send_o, recv_o, send2, recv2,
):
    staged = [
        pltpu.make_async_copy(src, dst, stage.at[k])
        for k, (src, dst) in enumerate(
            ((orient_hbm, orient_ref), (proj_hbm, proj_ref), (ctf_hbm, ctf_ref), (table_hbm, table_ref))
        )
    ]
    for copy in staged:
        copy.start()
    rep = lax.axis_index("rep")
    slab = lax.axis_index("slab")
    pix = lax.axis_index("pix")
    xc, core = rep // 2, rep % 2
    yc, zl = slab // 4, slab % 4
    zpos = pix * 4 + zl
    me = xc * 4 + yc
    sub = core * 2 + pix
    hub = core == 1
    mine = 1 - core

    def plane(q):
        return ((q // 4) * 2 + core, (q % 4) * 4 + zl, pix)

    def along_z(step):
        z = (zpos + step + RING) % RING
        return (rep, yc * 4 + z % 4, z // 4)

    partner = (xc * 2 + 1 - core, slab, pix)

    barrier = pltpu.get_barrier_semaphore()

    def greet(k, carry):
        pl.semaphore_signal(
            barrier, inc=1, device_id=plane((me + k) % 16), device_id_type=MESH
        )
        return carry

    lax.fori_loop(1, 16, greet, 0)
    pl.semaphore_signal(barrier, inc=1, device_id=partner, device_id_type=MESH)

    @pl.when(hub)
    def _():
        for peer in (along_z(1), along_z(-1)):
            pl.semaphore_signal(barrier, inc=1, device_id=peer, device_id_type=MESH)


    acc[...] = jnp.zeros_like(acc)
    for copy in staged:
        copy.wait()

    samples = proj_ref[...].reshape(64, 512).astype(jnp.float32)
    weights = ctf_ref[...].reshape(64, 256).astype(jnp.float32)
    real, imag = samples[:, :256], samples[:, 256:]
    first = jnp.concatenate([real, weights], axis=0).T
    second = jnp.concatenate([imag, imag], axis=0).T

    column = lax.broadcasted_iota(jnp.int32, (256, 128), 0)
    lane = lax.broadcasted_iota(jnp.int32, (256, 128), 1)
    geometry = jnp.zeros((4, 128), jnp.float32)
    for n in range(4):
        row = table_ref[orient_ref[n]].astype(jnp.float32).astype(jnp.bfloat16)
        pick = (column == slab * 16 + lane % 16) & ((lane // 16) % 4 == n)
        geometry += jnp.dot(
            row, pick.astype(jnp.float32).astype(jnp.bfloat16), preferred_element_type=jnp.float32
        )
    facts = jnp.concatenate(
        [
            geometry[0:1], geometry[2:3], geometry[1:2], geometry[3:4],
            jnp.zeros((12, 128), jnp.float32),
        ],
        axis=0,
    )
    low_half = lax.broadcasted_iota(jnp.int32, (16, 128), 1) < 64
    for q in range(16):
        piece[q, 0:16, :] = first[16 * q : 16 * q + 16].astype(jnp.bfloat16)
        piece[q, 16:32, :] = jnp.where(
            low_half, second[16 * q : 16 * q + 16], facts
        ).astype(jnp.bfloat16)

    pl.semaphore_wait(barrier, 16 + 2 * core)

    def across(src, dst, send, recv, k, into):
        to = (me + k) % 16
        return pltpu.make_async_remote_copy(
            src_ref=src.at[to], dst_ref=dst.at[into], send_sem=send.at[to], recv_sem=recv.at[into],
            device_id=plane(to), device_id_type=MESH,
        )

    def start_across(src, dst, send, recv):
        for dx, dy in FARTHEST_FIRST:
            to = (xc + dx) % 4 * 4 + (yc + dy) % 4
            pltpu.make_async_remote_copy(
                src_ref=src.at[to], dst_ref=dst.at[me], send_sem=send.at[to], recv_sem=recv.at[me],
                device_id=plane(to), device_id_type=MESH,
            ).start()

    def land_across(*refs):
        def go(k, carry):
            across(*refs, k, (me - k + 16) % 16).wait_recv()
            return carry

        lax.fori_loop(1, 16, go, 0)

    def drain_across(*refs):
        def go(k, carry):
            across(*refs, k, me).wait_send()
            return carry

        lax.fori_loop(1, 16, go, 0)

    start_across(piece, landed, send1, recv1)
    landed[me] = piece[me]
    land_across(piece, landed, send1, recv1)

    half = lax.broadcasted_iota(jnp.int32, (32, 128), 1) < 64
    tables = []
    for j in range(8):
        a = landed[2 * j].astype(jnp.float32)
        b = landed[2 * j + 1].astype(jnp.float32)
        top = jnp.where(half, a, pltpu.roll(b, 64, 1)).astype(jnp.bfloat16)
        bottom = jnp.where(half, pltpu.roll(a, 64, 1), b)
        at = pl.ds(128 * (j % 2), 128)
        row = 16 + 48 * (j // 2)
        gath[mine, row : row + 32, at] = top
        gath[mine, row + 32 : row + 48, at] = bottom[0:16].astype(jnp.bfloat16)
        tables.append(bottom[16:20])
    gath[mine, 0:16, :] = jnp.concatenate(
        [
            jnp.concatenate([tables[2 * g][f : f + 1], tables[2 * g + 1][f : f + 1]], axis=1)
            for f in range(4)
            for g in range(4)
        ],
        axis=0,
    ).astype(jnp.bfloat16)

    def move(src, dst, rows, send, recv, to):
        at = pl.ds(rows[0], rows[1])
        return pltpu.make_async_remote_copy(
            src_ref=gath.at[src, at], dst_ref=gath.at[dst, at],
            send_sem=send, recv_sem=recv, device_id=to, device_id_type=MESH,
        )

    def slots(side, t, part):
        return (FAR if t == 4 else slot_of(side, t)) + part // 2

    def index(side, t, part):
        return 16 * side + 4 * (t - 1) + part

    def ringed(side, t, part):
        src = part // 2 if t == 1 else slot_of(side, t - 1) + part // 2
        k = index(side, t, part)
        return move(
            src, slots(side, t, part), HALVES[part % 2], send_z.at[k], recv_z.at[k],
            along_z(1 - 2 * side),
        )

    def shared(side, t, part):
        slot, k = slots(side, t, part), index(side, t, part)
        return move(slot, slot, HALVES[part % 2], send_p.at[k], recv_z.at[k], partner)

    def exchanged(part):
        return move(mine, mine, HALVES[part], send_o.at[part], recv_o.at[part], partner)

    def arrive_partner(part):
        exchanged(part).wait_recv()

        @pl.when(hub)
        def _():
            for side in range(2):
                ringed(side, 1, 2 + part).start()

    def arrive(side, t, part):
        ringed(side, t, part).wait_recv()

        @pl.when(hub)
        def _():
            if t < 3:
                ringed(side, t + 1, part).start()
            shared(side, t, part).start()

        if t == 3:

            @pl.when(hub & (side == part % 2))
            def _():
                ringed(part % 2, 4, part).start()

    row16 = lax.broadcasted_iota(jnp.int32, (16, 256), 0).astype(jnp.float32)

    def operands(block, g, keys, lows, shares):
        def spread(v):
            return jnp.broadcast_to(v[g : g + 1], (16, 256)).astype(jnp.bfloat16)

        base = 16 + 48 * g
        zero = jnp.zeros((16, 256), jnp.bfloat16)
        pairs = []
        for i in range(2):
            x_low = spread(lows[i])
            key = [spread(keys[i][j]) for j in range(2)]
            share = [spread(shares[i][j]) for j in range(2)]
            right_side = []
            for t in range(16):
                here = (row16 + 16.0 * t).astype(jnp.bfloat16)
                right_side.append(
                    jnp.where(key[0] == here, share[0], jnp.where(key[1] == here, share[1], zero))
                )
            left_side = []
            for v in range(16):
                hit = x_low == jnp.full((16, 256), v, jnp.bfloat16)
                for c in range(3):
                    left_side.append(
                        jnp.where(hit, block[base + 16 * c : base + 16 * c + 16], zero)
                    )
            pairs.append((left_side, jnp.concatenate(right_side, axis=0)))
        return pairs

    def nt(a, b):
        return lax.dot_general(a, b, (((1,), (1,)), ((), ())), preferred_element_type=jnp.float32)

    def factors(slot):
        block = gath[slot]
        facts = block[0:16].astype(jnp.float32)
        x0, z0 = facts[0:4].astype(jnp.int32), facts[4:8].astype(jnp.int32)
        fx, fz = facts[8:12] / 256.0, facts[12:16] / 256.0
        keys, lows, shares = [], [], []
        for i in range(2):
            xr = x0 + i
            x_ok = ((xr >> 4) & 3) == sub
            lows.append((xr & 15).astype(jnp.float32))
            keys.append([])
            shares.append([])
            for j in range(2):
                zr = z0 + j
                ok = x_ok & (((zr >> 4) & 3) == zl)
                key = jnp.where(ok, (xr >> 6) * 64 + (zr >> 6) * 16 + (zr & 15), -1)
                keys[i].append(key.astype(jnp.float32))
                shares[i].append((fx if i else 1.0 - fx) * (fz if j else 1.0 - fz))
        pairs = []
        for g in range(4):
            pairs += operands(block, g, keys, lows, shares)
        return pairs

    def accumulate(*slots):
        pairs = []
        for slot in slots:
            pairs += factors(slot)
        for h in range(2):
            total = None
            for left_side, right_side in pairs:
                part = nt(jnp.concatenate(left_side[24 * h : 24 * h + 24], axis=0), right_side)
                total = part if total is None else total + part
            acc[pl.ds(384 * h, 384), :] += total

    near = jnp.where(zpos < 4, 1, 0)
    away = 1 - near

    @pl.when(hub)
    def _():
        for part in range(2):
            for side in range(2):
                ringed(side, 1, part).start()

    for part in range(2):
        exchanged(part).start()
    accumulate(mine)
    arrive_partner(0)
    arrive_partner(1)
    accumulate(core)
    arrive(near, 1, 0)
    arrive(near, 1, 1)
    accumulate(slot_of(near, 1))
    arrive(near, 1, 2)
    arrive(near, 1, 3)
    accumulate(slot_of(near, 1) + 1)
    arrive(away, 1, 0)
    arrive(away, 1, 1)
    accumulate(slot_of(away, 1))
    arrive(away, 1, 2)
    arrive(away, 1, 3)
    accumulate(slot_of(away, 1) + 1)
    arrive(near, 2, 0)
    arrive(away, 2, 0)
    arrive(near, 2, 1)
    arrive(away, 2, 1)
    accumulate(slot_of(near, 2))
    arrive(near, 2, 2)
    arrive(away, 2, 2)
    accumulate(slot_of(away, 2))
    arrive(near, 2, 3)
    arrive(away, 2, 3)
    arrive(near, 3, 0)
    accumulate(slot_of(near, 2) + 1)
    arrive(near, 3, 1)
    accumulate(slot_of(away, 2) + 1)
    arrive(near, 3, 2)
    accumulate(slot_of(near, 3))
    arrive(away, 3, 0)
    arrive(near, 3, 3)
    arrive(away, 3, 1)
    accumulate(slot_of(near, 3) + 1)
    arrive(away, 3, 2)
    arrive(away, 3, 3)
    accumulate(slot_of(away, 3))
    accumulate(slot_of(away, 3) + 1)
    arrive(0, 4, 0)
    arrive(1, 4, 1)
    accumulate(FAR)
    arrive(0, 4, 2)
    arrive(1, 4, 3)
    accumulate(FAR + 1)

    rows = []
    for v in range(16):
        base = 48 * v
        bottom = acc[pl.ds(base + 32, 16), :] + 1.0
        rows.append(acc[pl.ds(base, 16), :] / bottom)
        rows.append(acc[pl.ds(base + 16, 16), :] / bottom)
    for m in range(4):
        turned = jnp.concatenate(rows[8 * m : 8 * m + 8], axis=0).T
        for o in range(16):
            outbuf[o, :, pl.ds(128 * m, 128)] = turned[16 * o : 16 * o + 16].astype(jnp.bfloat16)

    start_across(outbuf, back, send2, recv2)
    back[me] = outbuf[me]
    land_across(outbuf, back, send2, recv2)

    lanes = lax.broadcasted_iota(jnp.int32, (16, 128), 1) // 16
    for m in range(4):
        for high in range(2):
            tiles = [back[8 * high + k, :, pl.ds(128 * m, 128)].astype(jnp.float32) for k in range(8)]
            for bit in (1, 2, 4):
                clear = (lanes & bit) == 0
                fresh = list(tiles)
                for k in range(8):
                    if k & bit == 0:
                        a, b = tiles[k], tiles[k | bit]
                        fresh[k] = jnp.where(clear, a, pltpu.roll(b, 16 * bit, 1))
                        fresh[k | bit] = jnp.where(clear, pltpu.roll(a, 128 - 16 * bit, 1), b)
                tiles = fresh
            for k in range(8):
                v, part = 4 * m + k // 2, k % 2
                out_ref[v, :, pl.ds(256 * part + 128 * high, 128)] = tiles[k].astype(jnp.bfloat16)

    drain_across(piece, landed, send1, recv1)
    for part in range(2):
        exchanged(part).wait_send()

    @pl.when(hub)
    def _():
        for side in range(2):
            for t in range(1, 5):
                for part in range(4) if t < 4 else (side, 2 + side):
                    ringed(side, t, part).wait_send()
                    shared(side, t, part).wait_send()

    drain_across(outbuf, back, send2, recv2)


def body(projections, ctf_weight, orient, angle_table):
    dma = pltpu.SemaphoreType.DMA
    return pl.pallas_call(
        kernel,
        out_shape=jax.ShapeDtypeStruct((16, 16, 512), jnp.bfloat16),
        in_specs=[pl.BlockSpec(memory_space=pltpu.HBM)] * 4,
        out_specs=pl.BlockSpec(memory_space=pltpu.VMEM),
        scratch_shapes=[
            pltpu.SMEM((4,), jnp.int32),
            pltpu.VMEM((4, 16, 512), jnp.bfloat16),
            pltpu.VMEM((4, 16, 256), jnp.bfloat16),
            pltpu.VMEM((64, 4, 256), jnp.int32),
            dma((4,)),
            pltpu.VMEM((16, 32, 128), jnp.bfloat16),
            pltpu.VMEM((16, 32, 128), jnp.bfloat16),
            pltpu.VMEM((16, 208, 256), jnp.bfloat16),
            pltpu.VMEM((768, 256), jnp.float32),
            pltpu.VMEM((16, 16, 512), jnp.bfloat16),
            pltpu.VMEM((16, 16, 512), jnp.bfloat16),
            dma((16,)), dma((16,)),
            dma((32,)), dma((32,)), dma((32,)), dma((2,)), dma((2,)),
            dma((16,)), dma((16,)),
        ],
        compiler_params=pltpu.CompilerParams(
            collective_id=0, has_side_effects=True, vmem_limit_bytes=67043328
        ),
    )(orient, projections, ctf_weight, angle_table).astype(jnp.float32)


def solution(mesh):
    placed = (
        P(("rep", "pix"), "slab", None),
        P(("rep", "pix"), "slab", None),
        P(("rep", "pix")),
        P(),
    )
    return jax.shard_map(
        body, mesh=mesh, in_specs=placed, out_specs=P(("rep", "pix"), "slab", None), check_vma=False
    )
```
